512 devices in a mesh: sec: 32 (over y, x), pan: 16 (over z, core).
Axes of the slice: x: 4, y: 8, z: 8, core: 2. Of those that a mesh axis runs over, the one named last changes fastest.
Arguments:
- wave_state: bfloat16 [32, 512, 512], P('sec', 'pan'), may hold values from -6 to 6
- right_blocks: bfloat16 [32, 16, 512, 512], P('sec', None, None, 'pan'), may hold values from -0.25 to 0.25
- left_blocks: bfloat16 [2304, 512, 512], P('sec', 'pan'), may hold values from -0.125 to 0.125
- coupling: bfloat16 [2304], P('sec'), may hold values from -1 to 1
- channel_term: int32 [2304], P('sec'), may hold values from 0 to 15
- channel_out: int32 [2304], P('sec'), may hold values from 0 to 31, as said below
- sector_dims: int32 [32], P('sec'), may hold values from 128 to 512
Outputs:
- applied: float32 [32, 512, 512], P('sec', 'pan')
The draws below stay inside these ranges and needn't reach their ends.
Inputs may be any that keep to these rules, and one draw needn't show every extreme that they name: `channel_out`: channel c ends in a sector at most two away from the sector c // 72 that it starts from.
All inputs are finite; a program needn't handle non-finite values.
Results may differ from the reference program's by a relative error of at most 0.0041.
Values may be sent and summed in bfloat16 or wider, within the bound.
A program may use at most 64 MiB of HBM per device.

```python
import jax
import jax.numpy as jnp
from jax import lax

DB = 512
NW = 16
CH_DEV = 72
SECTORS = 32
CHANNELS = 2304


def draw_channel_out(key, part):
    chan_total = CH_DEV * SECTORS
    source = jnp.arange(chan_total, dtype=jnp.int32) // CH_DEV
    offset = jax.random.randint(key, (chan_total,), -2, 3, dtype=jnp.int32)
    return jnp.clip(source + offset, 0, SECTORS - 1).astype(jnp.int32)


def place_ends(drawn, stream_key, low, largest):
    longest = drawn.shape.index(max(drawn.shape))
    spots = []
    for shift in (0, 1):
        where = [jax.random.randint(jax.random.fold_in(stream_key, axis), (), 0, length) for axis, length in enumerate(drawn.shape)]
        where[longest] = (where[longest] + shift) % drawn.shape[longest]
        spots.append(tuple(where))
    return drawn.at[spots[0]].set(low).at[spots[1]].set(largest)


def block_scale(own_key, shape, pieces, smallest, largest):
    factor_of = 1.0
    for position, shards_of in pieces:
        draws = jax.random.uniform(jax.random.fold_in(jax.random.fold_in(own_key, 6), position), (shards_of,), jnp.float32, smallest / len(pieces), largest / len(pieces))
        factor_of = factor_of * jnp.repeat(jnp.exp(draws), shape[position] // shards_of).reshape((-1,) + (1,) * (len(shape) - 1 - position))
    return factor_of


def bell_draw(rng, extent, spread, reach, shards=(), kind=jnp.bfloat16):
    gain = block_scale(rng, extent, shards, -0.22, 0.18) if shards else 1.0
    drawn = jax.random.normal(rng, extent, jnp.float32) * spread * gain
    return jnp.minimum(jnp.maximum(drawn, -reach), reach).astype(kind)


def setup_inputs(seed: int = 0) -> dict:
    streams_of = jax.random.split(jax.random.key(seed), 8)
    return {
        "wave_state": bell_draw(streams_of[0], (SECTORS, DB, DB), 1.0, 6.0, ((0, 32), (1, 16))),
        "right_blocks": bell_draw(streams_of[1], (SECTORS, NW, DB, DB), DB ** -0.5, 0.25, ((0, 32), (3, 16))),
        "left_blocks": bell_draw(streams_of[2], (CHANNELS, DB, DB), (4 * DB) ** -0.5, 0.125, ((0, 32), (1, 16))),
        "coupling": jnp.clip(jax.random.uniform(streams_of[3], (CHANNELS,), jnp.float32, -1.0, 1.0) * block_scale(streams_of[3], (CHANNELS,), ((0, 32),), -0.4, 0.0), -1.0, 1.0).astype(jnp.bfloat16),
        "channel_term": place_ends(jax.random.randint(streams_of[4], (CHANNELS,), 0, NW), jax.random.fold_in(streams_of[4], 1), 0, NW - 1).astype(jnp.int32),
        "channel_out": draw_channel_out(jax.random.fold_in(streams_of[7], 71), 0),
        "sector_dims": place_ends(jax.random.randint(streams_of[6], (SECTORS,), DB // 4, DB + 1), jax.random.fold_in(streams_of[6], 1), DB // 4, DB).astype(jnp.int32),
    }


def reference(wave_state, right_blocks, left_blocks, coupling, channel_term, channel_out, sector_dims):
    indices = jnp.arange(DB, dtype=jnp.int32)
    slot_ids = jnp.arange(5, dtype=jnp.int32)
    term_ids = jnp.arange(NW, dtype=jnp.int32)

    def visit_sector(totals, sector):
        live_dim = sector_dims[sector]
        inside = (indices[:, None] < live_dim) & (indices[None, :] < live_dim)
        masked = jnp.where(inside, wave_state[sector], jnp.zeros((), jnp.bfloat16))
        terms_here = jnp.einsum("ik,wkq->wiq", masked.astype(jnp.float32), right_blocks[sector].astype(jnp.float32)).astype(jnp.bfloat16)
        first_chan = (sector * CH_DEV).astype(jnp.int32)
        left_part = lax.dynamic_slice_in_dim(left_blocks, first_chan, CH_DEV, 0)
        coef_part = lax.dynamic_slice_in_dim(coupling, first_chan, CH_DEV, 0)
        kind_part = lax.dynamic_slice_in_dim(channel_term, first_chan, CH_DEV, 0)
        targets = lax.dynamic_slice_in_dim(channel_out, first_chan, CH_DEV, 0)
        slot_index = targets - sector + 2
        chosen = (slot_index[None, None, :] == slot_ids[:, None, None]) & (kind_part[None, None, :] == term_ids[None, :, None])
        weights = jnp.where(chosen, coef_part[None, None, :], jnp.zeros((), jnp.bfloat16)).reshape(5 * NW, CH_DEV)
        combined = jnp.dot(weights, left_part.reshape(CH_DEV, DB * DB), preferred_element_type=jnp.float32)
        combined = combined.astype(jnp.bfloat16).reshape(5, NW, DB, DB)
        partial_value = jnp.einsum("jwri,wiq->jrq", combined.astype(jnp.float32), terms_here.astype(jnp.float32))
        window = lax.dynamic_slice_in_dim(totals, sector, 5, 0)
        totals = lax.dynamic_update_slice_in_dim(totals, window + partial_value, sector, 0)
        return totals, None

    start_totals = jnp.zeros((SECTORS + 4, DB, DB), jnp.float32)
    totals, _ = lax.scan(visit_sector, start_totals, jnp.arange(SECTORS, dtype=jnp.int32))
    summed = totals[2:SECTORS + 2]
    limits = sector_dims[:, None, None]
    kept_mask = (indices[None, :, None] < limits) & (indices[None, None, :] < limits)
    return jnp.where(kept_mask, summed, jnp.zeros((), jnp.float32))
```

```python
import jax
import jax.numpy as jnp
from jax import lax
from jax.experimental import pallas as pl
from jax.experimental.pallas import tpu as pltpu
from jax.sharding import PartitionSpec as P

MESH = pl.DeviceIdType.MESH
F32 = jnp.float32
BF16 = jnp.bfloat16
OFFSETS = (-2, -1, 1, 2)
CHUNKS = 8


def nt_dot(lhs, rhs):
    return lax.dot_general(lhs, rhs, (((1,), (1,)), ((), ())), preferred_element_type=F32)


def kernel(
    state, right, left, coup, term, outc, dims,
    out_ref,
    ring, mbuf, mfull, lbuf, cbuf, xbuf, part, acc4, inbox, last, inlast,
    vcoup, vterm, vout, sdims,
    local_sem, s_send, s_recv, r_send, r_recv, pair_send, pair_recv,
    x_send, x_recv, a_send, a_recv, b_send, b_recv,
):
    sectors = lax.axis_size("sec")
    panels = lax.axis_size("pan")
    ring_size = panels // 2
    terms, cols, width = right.shape
    channels, rows, _ = left.shape
    sec = lax.axis_index("sec")
    pan = lax.axis_index("pan")
    zed = pan // 2
    core = lax.rem(pan, 2)
    partner = pan + 1 - 2 * core
    ahead = lax.rem(pan + 2, panels)
    behind = lax.rem(pan + panels - 2, panels)
    half = rows // 2
    per_chunk = terms // CHUNKS

    def sector_at(offset):
        return lax.rem(sec + offset + sectors, sectors)

    copy_right = pltpu.make_async_copy(right, ring.at[0], local_sem.at[0])
    copy_state = pltpu.make_async_copy(state.at[0], mbuf.at[pan], local_sem.at[1])
    copy_left = [
        pltpu.make_async_copy(left.at[:, pl.ds(g * half, half), :], lbuf.at[g], local_sem.at[2 + g])
        for g in range(2)
    ]
    tables = [
        pltpu.make_async_copy(coup, vcoup, local_sem.at[4]),
        pltpu.make_async_copy(term, vterm, local_sem.at[5]),
        pltpu.make_async_copy(outc, vout, local_sem.at[6]),
        pltpu.make_async_copy(dims, sdims, local_sem.at[7]),
    ]
    copy_state.start()
    copy_right.start()
    for copy in tables:
        copy.start()
    for copy in copy_left:
        copy.start()

    barrier = pltpu.get_barrier_semaphore()
    peers = [(sec, ahead), (sec, behind), (sec, partner)]
    for offset in OFFSETS:
        for other in (pan, partner):
            peers.append((sector_at(offset), other))
    for peer in peers:
        pl.semaphore_signal(barrier, inc=1, device_id=peer, device_id_type=MESH)

    for copy in tables:
        copy.wait()
    live = sdims[0]
    lanes = channels * half
    slot_row = (vout[...] - sec + 2).astype(F32)
    table = jnp.concatenate(
        [slot_row, vterm[...].astype(F32), vcoup[...].astype(F32), jnp.zeros((5, channels), F32)], axis=0
    ).astype(BF16)
    chan_of_lane = lax.broadcasted_iota(jnp.int32, (channels, lanes), 1) // half
    chan = lax.broadcasted_iota(jnp.int32, (channels, lanes), 0)
    spread = jnp.where(chan_of_lane == chan, 1.0, 0.0).astype(BF16)
    wide = jnp.dot(table, spread, preferred_element_type=F32)
    row_in_half = lax.rem(lax.broadcasted_iota(jnp.int32, (1, lanes), 1), half).astype(F32)
    target = (wide[1:2] * 5.0 + wide[0:1]) * float(half) + row_in_half
    weight = wide[2:3]

    pl.semaphore_wait(barrier, len(peers))

    def state_hop(way, dist, part_rows, index):
        sign = 1 if way == 0 else -1
        owner = lax.rem(pan - sign * 2 * (dist - 1) + panels, panels)
        return pltpu.make_async_remote_copy(
            src_ref=mbuf.at[owner, part_rows],
            dst_ref=mbuf.at[owner, part_rows],
            send_sem=s_send.at[way, index],
            recv_sem=s_recv.at[way, index],
            device_id=(sec, ahead if way == 0 else behind),
            device_id_type=MESH,
        )

    def state_arrival(way, dist, part_rows, index):
        sign = 1 if way == 0 else -1
        owner = lax.rem(pan - sign * 2 * dist + 2 * panels, panels)
        return pltpu.make_async_remote_copy(
            src_ref=mbuf.at[owner, part_rows],
            dst_ref=mbuf.at[owner, part_rows],
            send_sem=s_send.at[way, index],
            recv_sem=s_recv.at[way, index],
            device_id=(sec, ahead if way == 0 else behind),
            device_id_type=MESH,
        )

    def state_rows(way, dist):
        if dist < 4:
            return pl.ds(0, rows)
        return pl.ds(way * half, half)

    def slot(way, dist):
        if dist == 0:
            return 0
        return ring_size - dist if way == 0 else dist

    def ring_hop(way, dist, chunk):
        piece = pl.ds(chunk * per_chunk, per_chunk)
        return pltpu.make_async_remote_copy(
            src_ref=ring.at[slot(way, dist - 1), piece],
            dst_ref=ring.at[slot(way, dist), piece],
            send_sem=r_send.at[way, dist - 1, chunk],
            recv_sem=r_recv.at[way, dist - 1, chunk],
            device_id=(sec, ahead if way == 0 else behind),
            device_id_type=MESH,
        )

    def carried(way, dist, chunk):
        return dist < 4 or (chunk < CHUNKS // 2) == (way == 0)

    sends = []

    def go(copy):
        copy.start()
        sends.append(copy)

    def send_state(dist):
        for way in range(2):
            go(state_hop(way, dist, state_rows(way, dist), dist - 1))

    def wait_state(dist):
        for way in range(2):
            state_arrival(way, dist, state_rows(way, dist), dist - 1).wait_recv()

    def send_own(chunks):
        for chunk in chunks:
            for way in range(2):
                go(ring_hop(way, 1, chunk))

    def service(dist, chunks):
        for chunk in chunks:
            for way in range(2):
                if carried(way, dist, chunk):
                    ring_hop(way, dist, chunk).wait_recv()
                    if dist < 4 and carried(way, dist + 1, chunk):
                        go(ring_hop(way, dist + 1, chunk))

    tile = 256

    def combine(step):
        at = lax.broadcasted_iota(jnp.int32, (tile, lanes), 0).astype(F32) + float(step * tile)
        kron = jnp.where(at == target, weight, 0.0).astype(BF16)
        for g in range(2):
            made = jnp.dot(kron, lbuf[g].reshape(lanes, width), preferred_element_type=F32).astype(BF16)
            groups = tile // half
            cbuf[pl.ds(step * groups, groups), g] = made.reshape(groups, half, width)

    copy_state.wait()
    send_state(1)
    copy_right.wait()
    send_own((0, 1))
    for copy in copy_left:
        copy.wait()
    combine(0)
    combine(1)
    wait_state(1)
    send_state(2)
    send_own((2, 3))
    combine(2)
    combine(3)
    wait_state(2)
    send_state(3)
    send_own((4, 5))
    combine(4)
    wait_state(3)
    send_state(4)
    send_own((6, 7))
    service(1, range(0, 2))
    wait_state(4)
    pair = []
    for step in range(ring_size):
        copy = pltpu.make_async_remote_copy(
            src_ref=mbuf.at[2 * step + core],
            dst_ref=mbuf.at[2 * step + core],
            send_sem=pair_send.at[step],
            recv_sem=pair_recv.at[step],
            device_id=(sec, partner),
            device_id_type=MESH,
        )
        pair.append(copy)
        go(copy)
    service(1, range(2, 4))
    for step in range(ring_size):
        pltpu.make_async_remote_copy(
            src_ref=mbuf.at[2 * step + 1 - core],
            dst_ref=mbuf.at[2 * step + 1 - core],
            send_sem=pair_send.at[step],
            recv_sem=pair_recv.at[step],
            device_id=(sec, partner),
            device_id_type=MESH,
        ).wait_recv()

    row_at = lax.broadcasted_iota(jnp.int32, (width, width), 0)
    col_at = lax.broadcasted_iota(jnp.int32, (width, width), 1)
    masked = jnp.where(
        (row_at < live) & (col_at < live), mbuf[...].reshape(width, width), jnp.zeros((), BF16)
    )
    mfull[...] = masked
    group = 4
    x_copies = []
    for step in range(terms // group):
        block = cbuf[pl.ds(step * group * 5, group * 5)].reshape(group * 5 * rows, width)
        made = jnp.dot(block, mfull[...], preferred_element_type=F32).astype(BF16)
        xbuf[pl.ds(step * group, group), core] = made.reshape(group, 5 * rows, width)
        service(1, (4 + step,))
        copy = pltpu.make_async_remote_copy(
            src_ref=xbuf.at[pl.ds(step * group, group), core],
            dst_ref=xbuf.at[pl.ds(step * group, group), core],
            send_sem=x_send.at[step],
            recv_sem=x_recv.at[step],
            device_id=(sec, partner),
            device_id_type=MESH,
        )
        x_copies.append(copy)
        go(copy)

    part[:, :, pl.ds(128, 128)] = jnp.zeros((10, rows, 128), F32)
    service(2, range(0, 2))
    for step in range(terms // group):
        pltpu.make_async_remote_copy(
            src_ref=xbuf.at[pl.ds(step * group, group), 1 - core],
            dst_ref=xbuf.at[pl.ds(step * group, group), 1 - core],
            send_sem=x_send.at[step],
            recv_sem=x_recv.at[step],
            device_id=(sec, partner),
            device_id_type=MESH,
        ).wait_recv()

    def contract(slots, which):
        total = None
        for w in which:
            blocks = [ring[k, w] for k in slots]
            block = blocks[0] if len(blocks) == 1 else jnp.concatenate(blocks, axis=0)
            product = nt_dot(xbuf[w].reshape(10 * rows, width), block)
            total = product if total is None else total + product
        return total

    def place(slots, total):
        for i, k in enumerate(slots):
            part[:, :, pl.ds(k * cols, cols)] = total[:, i * cols : (i + 1) * cols].reshape(10, rows, cols)

    place((0, 1, 7), contract((0, 1, 7), range(terms)))
    service(2, range(2, 8))
    place((2, 6), contract((2, 6), range(terms)))
    service(3, range(0, 8))
    place((3, 5), contract((3, 5), range(terms)))

    def by_final_step(step):
        low = [step * per_chunk + i for i in range(per_chunk)]
        return low + [terms // 2 + w for w in low]

    def final_wait(step):
        ring_hop(0, 4, step).wait_recv()
        ring_hop(1, 4, CHUNKS // 2 + step).wait_recv()

    final_wait(0)
    acc4[...] = contract((4,), by_final_step(0))

    def a_copy(which, j):
        return pltpu.make_async_remote_copy(
            src_ref=part.at[which * 5 + j],
            dst_ref=inbox.at[j, core],
            send_sem=a_send.at[which, j],
            recv_sem=a_recv.at[j, core],
            device_id=(sector_at(j - 2), 2 * zed + which),
            device_id_type=MESH,
        )

    def b_copy(which, j):
        return pltpu.make_async_remote_copy(
            src_ref=last.at[which * 5 + j],
            dst_ref=inlast.at[j, core],
            send_sem=b_send.at[which, j],
            recv_sem=b_recv.at[j, core],
            device_id=(sector_at(j - 2), 2 * zed + which),
            device_id_type=MESH,
        )

    order = [(which, j) for j in (0, 4, 1, 3) for which in (0, 1)]

    def spread_out(maker):
        copies = [maker(which, j) for which, j in order]
        copies.append(maker(1 - core, 2))
        for copy in copies:
            go(copy)

    def arrivals(target_ref, send_sem, recv_sem, source_ref):
        for j, cls in [(j, cls) for j in (0, 1, 3, 4) for cls in (0, 1)] + [(2, 1 - core)]:
            pltpu.make_async_remote_copy(
                src_ref=source_ref.at[0],
                dst_ref=target_ref.at[j, cls],
                send_sem=send_sem.at[0, j],
                recv_sem=recv_sem.at[j, cls],
                device_id=(sec, partner),
                device_id_type=MESH,
            ).wait_recv()

    spread_out(a_copy)
    for step in range(1, CHUNKS // 2 - 1):
        final_wait(step)
        acc4[...] = acc4[...] + contract((4,), by_final_step(step))
    final_wait(CHUNKS // 2 - 1)
    done = acc4[...] + contract((4,), by_final_step(CHUNKS // 2 - 1))
    done = done.reshape(10, rows // 8, 8, cols)
    packed = jnp.concatenate([done[:, i] for i in range(rows // 8)], axis=2)
    last[...] = packed
    spread_out(b_copy)

    arrivals(inbox, a_send, a_recv, part)
    inbox[2, core] = part[core * 5 + 2]
    inlast[2, core] = last[core * 5 + 2]
    sums = []
    for cls in range(2):
        total = inbox[0, cls]
        for j in range(1, 5):
            total = total + inbox[j, cls]
        sums.append(pltpu.roll(total, zed * cols, axis=1))
    pieces = []
    for k in range(ring_size):
        for cls in range(2):
            pieces.append(sums[cls][:, k * cols : (k + 1) * cols])
    early = jnp.concatenate(pieces, axis=1)
    lane = lax.broadcasted_iota(jnp.int32, (rows, width), 1)
    row = lax.broadcasted_iota(jnp.int32, (rows, width), 0) + pan * rows
    keep = (row < live) & (lane < live)
    here = lane // (2 * cols) == lax.rem(zed + 4, ring_size)

    arrivals(inlast, b_send, b_recv, last)
    lasts = []
    for cls in range(2):
        total = inlast[0, cls]
        for j in range(1, 5):
            total = total + inlast[j, cls]
        lasts.append(
            jnp.concatenate([total[:, i * cols : (i + 1) * cols] for i in range(rows // 8)], axis=0)
        )
    late = jnp.concatenate(lasts * (width // (2 * cols)), axis=1)
    out_ref[0] = jnp.where(keep, early + jnp.where(here, late, 0.0), 0.0)
    for copy in sends:
        copy.wait_send()


def on_device(
    wave_state, right_blocks, left_blocks, coupling, channel_term, channel_out, sector_dims
):
    _, rows, width = wave_state.shape
    _, terms, _, cols = right_blocks.shape
    channels = left_blocks.shape[0]
    panels = lax.axis_size("pan")
    ring_size = panels // 2
    half = rows // 2
    right = jnp.swapaxes(right_blocks[0], 1, 2)
    dma = pltpu.SemaphoreType.DMA
    return pl.pallas_call(
        kernel,
        out_shape=jax.ShapeDtypeStruct((1, rows, width), F32),
        in_specs=[pl.BlockSpec(memory_space=pl.ANY)] * 7,
        out_specs=pl.BlockSpec(memory_space=pltpu.VMEM),
        scratch_shapes=[
            pltpu.VMEM((ring_size, terms, cols, width), BF16),
            pltpu.VMEM((panels, rows, width), BF16),
            pltpu.VMEM((width, width), BF16),
            pltpu.VMEM((2, channels, half, width), BF16),
            pltpu.VMEM((5 * terms, 2, half, width), BF16),
            pltpu.VMEM((terms, 2, 5 * rows, width), BF16),
            pltpu.VMEM((10, rows, ring_size * cols), F32),
            pltpu.VMEM((10 * rows, cols), F32),
            pltpu.VMEM((5, 2, rows, ring_size * cols), F32),
            pltpu.VMEM((10, 8, rows // 8 * cols), F32),
            pltpu.VMEM((5, 2, 8, rows // 8 * cols), F32),
            pltpu.VMEM((1, channels), BF16),
            pltpu.VMEM((1, channels), jnp.int32),
            pltpu.VMEM((1, channels), jnp.int32),
            pltpu.SMEM((1,), jnp.int32),
            dma((8,)),
            dma((2, 4)),
            dma((2, 4)),
            dma((2, 4, CHUNKS)),
            dma((2, 4, CHUNKS)),
            dma((ring_size,)),
            dma((ring_size,)),
            dma((4,)),
            dma((4,)),
            dma((2, 5)),
            dma((5, 2)),
            dma((2, 5)),
            dma((5, 2)),
        ],
        compiler_params=pltpu.CompilerParams(
            collective_id=0, has_side_effects=True, vmem_limit_bytes=60 * 1024 * 1024
        ),
        name="sector_step",
    )(
        wave_state,
        right,
        left_blocks,
        coupling[None],
        channel_term[None],
        channel_out[None],
        sector_dims,
    )


def solution(mesh):
    return jax.shard_map(
        on_device,
        mesh=mesh,
        in_specs=(
            P("sec", "pan", None),
            P("sec", None, None, "pan"),
            P("sec", "pan", None),
            P("sec"),
            P("sec"),
            P("sec"),
            P("sec"),
        ),
        out_specs=P("sec", "pan", None),
        check_vma=False,
    )
```

```python
import jax
import jax.numpy as jnp
from jax import lax
from jax.experimental import pallas as pl
from jax.experimental.pallas import tpu as pltpu
from jax.sharding import PartitionSpec as P

MESH = pl.DeviceIdType.MESH
F32 = jnp.float32
BF16 = jnp.bfloat16
OFFSETS = (-2, -1, 1, 2)
CHUNKS = 8


def nt_dot(lhs, rhs):
    return lax.dot_general(lhs, rhs, (((1,), (1,)), ((), ())), preferred_element_type=F32)


def kernel(
    state, right, left, coup, term, outc, dims,
    out_ref,
    ring, mbuf, mfull, lbuf, cbuf, xbuf, part, acc2, acc3, acc4, inbox, mid, inmid, last, inlast,
    vcoup, vterm, vout, sdims,
    local_sem, s_send, s_recv, r_send, r_recv, pair_send, pair_recv,
    x_send, x_recv, a_send, a_recv, m_send, m_recv, b_send, b_recv,
):
    sectors = lax.axis_size("sec")
    panels = lax.axis_size("pan")
    ring_size = panels // 2
    terms, cols, width = right.shape
    channels, rows, _ = left.shape
    sec = lax.axis_index("sec")
    pan = lax.axis_index("pan")
    zed = pan // 2
    core = lax.rem(pan, 2)
    partner = pan + 1 - 2 * core
    ahead = lax.rem(pan + 2, panels)
    behind = lax.rem(pan + panels - 2, panels)
    half = rows // 2
    per_chunk = terms // CHUNKS

    def sector_at(offset):
        return lax.rem(sec + offset + sectors, sectors)

    def has_sector(offset):
        return (sec + offset >= 0) & (sec + offset < sectors)

    copy_right = pltpu.make_async_copy(right, ring.at[0], local_sem.at[0])
    copy_state = pltpu.make_async_copy(state.at[0], mbuf.at[pan], local_sem.at[1])
    copy_left = [
        pltpu.make_async_copy(left.at[:, pl.ds(g * half, half), :], lbuf.at[g], local_sem.at[2 + g])
        for g in range(2)
    ]
    tables = [
        pltpu.make_async_copy(coup, vcoup, local_sem.at[4]),
        pltpu.make_async_copy(term, vterm, local_sem.at[5]),
        pltpu.make_async_copy(outc, vout, local_sem.at[6]),
        pltpu.make_async_copy(dims, sdims, local_sem.at[7]),
    ]
    copy_state.start()
    copy_right.start()
    for copy in tables:
        copy.start()
    for copy in copy_left:
        copy.start()

    barrier = pltpu.get_barrier_semaphore()
    for peer in (ahead, behind, partner):
        pl.semaphore_signal(barrier, inc=1, device_id=(sec, peer), device_id_type=MESH)
    greeted = 3
    for offset in OFFSETS:
        exists = has_sector(offset)
        greeted = greeted + 2 * jnp.where(exists, 1, 0)

        @pl.when(exists)
        def _():
            for other in (pan, partner):
                pl.semaphore_signal(
                    barrier, inc=1, device_id=(sector_at(offset), other), device_id_type=MESH
                )

    with jax.named_scope("barrier"):
        pl.semaphore_wait(barrier, greeted)

    for offset in OFFSETS:

        @pl.when(jnp.logical_not(has_sector(-offset)))
        def _():
            inbox[offset + 2] = jnp.zeros(inbox.shape[1:], F32)
            inmid[offset + 2] = jnp.zeros(inmid.shape[1:], F32)
            inlast[offset + 2] = jnp.zeros(inlast.shape[1:], F32)

    def state_hop(way, dist, part_rows, index):
        sign = 1 if way == 0 else -1
        owner = lax.rem(pan - sign * 2 * (dist - 1) + panels, panels)
        return pltpu.make_async_remote_copy(
            src_ref=mbuf.at[owner, part_rows],
            dst_ref=mbuf.at[owner, part_rows],
            send_sem=s_send.at[way, index],
            recv_sem=s_recv.at[way, index],
            device_id=(sec, ahead if way == 0 else behind),
            device_id_type=MESH,
        )

    def state_arrival(way, dist, part_rows, index):
        sign = 1 if way == 0 else -1
        owner = lax.rem(pan - sign * 2 * dist + 2 * panels, panels)
        return pltpu.make_async_remote_copy(
            src_ref=mbuf.at[owner, part_rows],
            dst_ref=mbuf.at[owner, part_rows],
            send_sem=s_send.at[way, index],
            recv_sem=s_recv.at[way, index],
            device_id=(sec, ahead if way == 0 else behind),
            device_id_type=MESH,
        )

    def state_rows(way, dist):
        if dist < 4:
            return pl.ds(0, rows)
        return pl.ds(way * half, half)

    def slot(way, dist):
        if dist == 0:
            return 0
        return ring_size - dist if way == 0 else dist

    def ring_hop(way, dist, chunk):
        piece = pl.ds(chunk * per_chunk, per_chunk)
        return pltpu.make_async_remote_copy(
            src_ref=ring.at[slot(way, dist - 1), piece],
            dst_ref=ring.at[slot(way, dist), piece],
            send_sem=r_send.at[way, dist - 1, chunk],
            recv_sem=r_recv.at[way, dist - 1, chunk],
            device_id=(sec, ahead if way == 0 else behind),
            device_id_type=MESH,
        )

    def carried(way, dist, chunk):
        return dist < 4 or (chunk < CHUNKS // 2) == (way == 0)

    sends = []

    def go(copy):
        copy.start()
        sends.append(copy)

    def send_state(dist):
        for way in range(2):
            go(state_hop(way, dist, state_rows(way, dist), dist - 1))

    def wait_state(dist):
        for way in range(2):
            state_arrival(way, dist, state_rows(way, dist), dist - 1).wait_recv()

    def send_own(chunks):
        for chunk in chunks:
            for way in range(2):
                go(ring_hop(way, 1, chunk))

    def service(dist, chunks):
        for chunk in chunks:
            for way in range(2):
                if carried(way, dist, chunk):
                    ring_hop(way, dist, chunk).wait_recv()
                    if dist < 4 and carried(way, dist + 1, chunk):
                        go(ring_hop(way, dist + 1, chunk))

    with jax.named_scope("own_state"):
        copy_state.wait()
        send_state(1)
    with jax.named_scope("own_right"):
        copy_right.wait()
        send_own((0, 1))

    for copy in tables:
        copy.wait()
    live = sdims[0, 0]
    lanes = channels * half
    slot_row = (vout[...] - sec + 2).astype(F32)
    table = jnp.concatenate(
        [slot_row, vterm[...].astype(F32), vcoup[...].astype(F32), jnp.zeros((5, channels), F32)], axis=0
    ).astype(BF16)
    chan_of_lane = lax.broadcasted_iota(jnp.int32, (channels, lanes), 1) // half
    chan = lax.broadcasted_iota(jnp.int32, (channels, lanes), 0)
    spread = jnp.where(chan_of_lane == chan, 1.0, 0.0).astype(BF16)
    wide = jnp.dot(table, spread, preferred_element_type=F32)
    row_in_half = lax.rem(lax.broadcasted_iota(jnp.int32, (1, lanes), 1), half).astype(F32)
    target = (wide[1:2] * 5.0 + wide[0:1]) * float(half) + row_in_half
    weight = wide[2:3]

    tile = 256

    def combine(step):
        at = lax.broadcasted_iota(jnp.int32, (tile, lanes), 0).astype(F32) + float(step * tile)
        kron = jnp.where(at == target, weight, 0.0).astype(BF16)
        for g in range(2):
            made = jnp.dot(kron, lbuf[g].reshape(lanes, width), preferred_element_type=F32).astype(BF16)
            groups = tile // half
            cbuf[pl.ds(step * groups, groups), g] = made.reshape(groups, half, width)

    for copy in copy_left:
        copy.wait()
    with jax.named_scope("combine_a"):
        combine(0)
        combine(1)
    with jax.named_scope("hop_1"):
        wait_state(1)
    send_state(2)
    send_own((2, 3))
    combine(2)
    combine(3)
    with jax.named_scope("hop_2"):
        wait_state(2)
    send_state(3)
    send_own((4, 5))
    combine(4)
    with jax.named_scope("hop_3"):
        wait_state(3)
    send_state(4)
    send_own((6, 7))
    service(1, range(0, 2))
    with jax.named_scope("hop_4"):
        wait_state(4)
    pair = []
    for step in range(ring_size):
        copy = pltpu.make_async_remote_copy(
            src_ref=mbuf.at[2 * step + core],
            dst_ref=mbuf.at[2 * step + core],
            send_sem=pair_send.at[step],
            recv_sem=pair_recv.at[step],
            device_id=(sec, partner),
            device_id_type=MESH,
        )
        pair.append(copy)
        go(copy)
    service(1, range(2, 4))
    for step in range(ring_size):
        pltpu.make_async_remote_copy(
            src_ref=mbuf.at[2 * step + 1 - core],
            dst_ref=mbuf.at[2 * step + 1 - core],
            send_sem=pair_send.at[step],
            recv_sem=pair_recv.at[step],
            device_id=(sec, partner),
            device_id_type=MESH,
        ).wait_recv()

    row_at = lax.broadcasted_iota(jnp.int32, (width, width), 0)
    col_at = lax.broadcasted_iota(jnp.int32, (width, width), 1)
    masked = jnp.where(
        (row_at < live) & (col_at < live), mbuf[...].reshape(width, width), jnp.zeros((), BF16)
    )
    mfull[...] = masked
    group = 4
    x_copies = []
    for step in range(terms // group):
        block = cbuf[pl.ds(step * group * 5, group * 5)].reshape(group * 5 * rows, width)
        made = jnp.dot(block, mfull[...], preferred_element_type=F32).astype(BF16)
        xbuf[pl.ds(step * group, group), core] = made.reshape(group, 5 * rows, width)
        service(1, (4 + step,))
        copy = pltpu.make_async_remote_copy(
            src_ref=xbuf.at[pl.ds(step * group, group), core],
            dst_ref=xbuf.at[pl.ds(step * group, group), core],
            send_sem=x_send.at[step],
            recv_sem=x_recv.at[step],
            device_id=(sec, partner),
            device_id_type=MESH,
        )
        x_copies.append(copy)
        go(copy)

    part[...] = jnp.zeros(part.shape, F32)
    for step in range(terms // group):
        pltpu.make_async_remote_copy(
            src_ref=xbuf.at[pl.ds(step * group, group), 1 - core],
            dst_ref=xbuf.at[pl.ds(step * group, group), 1 - core],
            send_sem=x_send.at[step],
            recv_sem=x_recv.at[step],
            device_id=(sec, partner),
            device_id_type=MESH,
        ).wait_recv()

    def contract(slots, which, held):
        blocks = []
        for w in which:
            pieces = [ring[k, w] for k in slots]
            blocks.append(pieces[0] if len(pieces) == 1 else jnp.concatenate(pieces, axis=0))
        totals = []
        for owner in range(2):
            total = None if held is None else held[owner]
            for w, block in zip(which, blocks):
                product = nt_dot(xbuf[w, owner], block)
                total = product if total is None else total + product
            totals.append(total)
        return totals

    def place(slots, totals):
        for owner, total in enumerate(totals):
            for i, k in enumerate(slots):
                piece = total[:, i * cols : (i + 1) * cols].reshape(5, rows, cols)
                part[pl.ds(owner * 5, 5), :, pl.ds(k * cols, cols)] = piece

    def keep_in(acc, totals):
        for owner, total in enumerate(totals):
            acc[owner] = total

    def pack(total):
        total = total.reshape(5, rows // 8, 8, cols)
        return jnp.concatenate([total[:, i] for i in range(rows // 8)], axis=2)

    def unpack(packed):
        return jnp.concatenate([packed[:, i * cols : (i + 1) * cols] for i in range(rows // 8)], axis=0)

    def exchange(source, landing, send_sem, recv_sem):
        def copy_to(which, j):
            return pltpu.make_async_remote_copy(
                src_ref=source.at[which * 5 + j],
                dst_ref=landing.at[j, core],
                send_sem=send_sem.at[which, j],
                recv_sem=recv_sem.at[j, core],
                device_id=(sector_at(j - 2), 2 * zed + which),
                device_id_type=MESH,
            )

        def copy_from(j, cls):
            return pltpu.make_async_remote_copy(
                src_ref=source.at[0],
                dst_ref=landing.at[j, cls],
                send_sem=send_sem.at[0, j],
                recv_sem=recv_sem.at[j, cls],
                device_id=(sec, partner),
                device_id_type=MESH,
            )

        def start():
            for j in (0, 4, 1, 3):

                @pl.when(has_sector(j - 2))
                def _():
                    for which in range(2):
                        copy_to(which, j).start()

            copy_to(1 - core, 2).start()

        def wait_recv():
            for j in (0, 4, 1, 3):

                @pl.when(has_sector(2 - j))
                def _():
                    for cls in range(2):
                        copy_from(j, cls).wait_recv()

            copy_from(2, 1 - core).wait_recv()

        def wait_send():
            for j in (0, 4, 1, 3):

                @pl.when(has_sector(j - 2))
                def _():
                    for which in range(2):
                        copy_to(which, j).wait_send()

            copy_to(1 - core, 2).wait_send()

        return start, wait_recv, wait_send

    def sum_of(landing, cls):
        total = landing[0, cls]
        for j in range(1, 5):
            total = total + landing[j, cls]
        return total

    start_a, recv_a, sent_a = exchange(part, inbox, a_send, a_recv)
    start_m, recv_m, sent_m = exchange(mid, inmid, m_send, m_recv)
    start_b, recv_b, sent_b = exchange(last, inlast, b_send, b_recv)

    def chunk_terms(chunk):
        return range(chunk * per_chunk, (chunk + 1) * per_chunk)

    with jax.named_scope("contract_a"):
        place((0, 1, 7), contract((0, 1, 7), range(terms), None))
    with jax.named_scope("ring_2"):
        for chunk in range(CHUNKS):
            service(2, (chunk,))
            if chunk % 2:
                both = range((chunk - 1) * per_chunk, (chunk + 1) * per_chunk)
                totals = contract((2, 6), both, acc2 if chunk > 1 else None)
                if chunk < CHUNKS - 1:
                    keep_in(acc2, totals)
                else:
                    place((2, 6), totals)
    with jax.named_scope("ring_3"):
        service(3, (0,))
        start_a()
        keep_in(acc3, contract((3, 5), chunk_terms(0), None))
        for chunk in range(1, CHUNKS):
            service(3, (chunk,))
            keep_in(acc3, contract((3, 5), chunk_terms(chunk), acc3))
        for owner in range(2):
            for i in range(2):
                mid[pl.ds(owner * 5, 5), pl.ds(8 * i, 8)] = pack(acc3[owner, :, pl.ds(i * cols, cols)])

    def by_final_step(step):
        low = list(chunk_terms(step))
        return low + [terms // 2 + w for w in low]

    def final_wait(step):
        ring_hop(0, 4, step).wait_recv()
        ring_hop(1, 4, CHUNKS // 2 + step).wait_recv()

    final_wait(0)
    start_m()
    keep_in(acc4, contract((4,), by_final_step(0), None))
    for step in range(1, CHUNKS // 2 - 1):
        final_wait(step)
        keep_in(acc4, contract((4,), by_final_step(step), acc4))
    with jax.named_scope("final_wait"):
        final_wait(CHUNKS // 2 - 1)
    with jax.named_scope("last"):
        totals = contract((4,), by_final_step(CHUNKS // 2 - 1), acc4)
        for owner in range(2):
            last[pl.ds(owner * 5, 5)] = pack(totals[owner])
        start_b()

    recv_a()
    inbox[2, core] = part[core * 5 + 2]
    inmid[2, core] = mid[core * 5 + 2]
    inlast[2, core] = last[core * 5 + 2]
    recv_m()
    sums = []
    for cls in range(2):
        total = sum_of(inbox, cls)
        extra = sum_of(inmid, cls)
        total = jnp.concatenate(
            [
                total[:, : 3 * cols],
                unpack(extra[:8]),
                total[:, 4 * cols : 5 * cols],
                unpack(extra[8:]),
                total[:, 6 * cols :],
            ],
            axis=1,
        )
        sums.append(pltpu.roll(total, zed * cols, axis=1))
    pieces = []
    for k in range(ring_size):
        for cls in range(2):
            pieces.append(sums[cls][:, k * cols : (k + 1) * cols])
    early = jnp.concatenate(pieces, axis=1)
    lane = lax.broadcasted_iota(jnp.int32, (rows, width), 1)
    here = lane // (2 * cols) == lax.rem(zed + 4, ring_size)
    with jax.named_scope("sent"):
        for copy in sends:
            copy.wait_send()
        sent_a()
        sent_m()
        sent_b()
    with jax.named_scope("recv_b"):
        recv_b()
    with jax.named_scope("finish"):
        lasts = [unpack(sum_of(inlast, cls)) for cls in range(2)]
        late = jnp.concatenate(lasts * (width // (2 * cols)), axis=1)
        out_ref[0] = early + jnp.where(here, late, 0.0)


def on_device(
    wave_state, right_blocks, left_blocks, coupling, channel_term, channel_out, sector_dims
):
    _, rows, width = wave_state.shape
    _, terms, _, cols = right_blocks.shape
    channels = left_blocks.shape[0]
    panels = lax.axis_size("pan")
    ring_size = panels // 2
    half = rows // 2
    right = jnp.swapaxes(right_blocks[0], 1, 2)
    dma = pltpu.SemaphoreType.DMA
    applied = pl.pallas_call(
        kernel,
        out_shape=jax.ShapeDtypeStruct((1, rows, width), F32),
        in_specs=[pl.BlockSpec(memory_space=pltpu.HBM)] * 7,
        out_specs=pl.BlockSpec(memory_space=pltpu.VMEM),
        scratch_shapes=[
            pltpu.VMEM((ring_size, terms, cols, width), BF16),
            pltpu.VMEM((panels, rows, width), BF16),
            pltpu.VMEM((width, width), BF16),
            pltpu.VMEM((2, channels, half, width), BF16),
            pltpu.VMEM((5 * terms, 2, half, width), BF16),
            pltpu.VMEM((terms, 2, 5 * rows, width), BF16),
            pltpu.VMEM((10, rows, ring_size * cols), F32),
            pltpu.VMEM((2, 5 * rows, 2 * cols), F32),
            pltpu.VMEM((2, 5 * rows, 2 * cols), F32),
            pltpu.VMEM((2, 5 * rows, cols), F32),
            pltpu.VMEM((5, 2, rows, ring_size * cols), F32),
            pltpu.VMEM((10, 16, rows // 8 * cols), F32),
            pltpu.VMEM((5, 2, 16, rows // 8 * cols), F32),
            pltpu.VMEM((10, 8, rows // 8 * cols), F32),
            pltpu.VMEM((5, 2, 8, rows // 8 * cols), F32),
            pltpu.VMEM((1, channels), BF16),
            pltpu.VMEM((1, channels), jnp.int32),
            pltpu.VMEM((1, channels), jnp.int32),
            pltpu.SMEM((1, 1), jnp.int32),
            dma((8,)),
            dma((2, 4)),
            dma((2, 4)),
            dma((2, 4, CHUNKS)),
            dma((2, 4, CHUNKS)),
            dma((ring_size,)),
            dma((ring_size,)),
            dma((4,)),
            dma((4,)),
            dma((2, 5)),
            dma((5, 2)),
            dma((2, 5)),
            dma((5, 2)),
            dma((2, 5)),
            dma((5, 2)),
        ],
        compiler_params=pltpu.CompilerParams(
            collective_id=0, has_side_effects=True, vmem_limit_bytes=60 * 1024 * 1024
        ),
        name="sector_step",
    )(
        wave_state,
        right,
        left_blocks,
        coupling[None],
        channel_term[None],
        channel_out[None],
        sector_dims[None],
    )
    live = sector_dims[0]
    row_ids = lax.axis_index("pan") * rows + lax.iota(jnp.int32, rows)
    kept_mask = (row_ids[:, None] < live) & (lax.iota(jnp.int32, width)[None, :] < live)
    return jnp.where(kept_mask[None], applied, jnp.zeros((), F32))


def solution(mesh):
    return jax.shard_map(
        on_device,
        mesh=mesh,
        in_specs=(
            P("sec", "pan", None),
            P("sec", None, None, "pan"),
            P("sec", "pan", None),
            P("sec"),
            P("sec"),
            P("sec"),
            P("sec"),
        ),
        out_specs=P("sec", "pan", None),
        check_vma=False,
    )
```

```python
import jax
import jax.numpy as jnp
from jax import lax
from jax.experimental import pallas as pl
from jax.experimental.pallas import tpu as pltpu
from jax.sharding import PartitionSpec as P

MESH = pl.DeviceIdType.MESH
F32 = jnp.float32
BF16 = jnp.bfloat16
OFFSETS = (-2, -1, 1, 2)
CHUNKS = 4
LAST_CHUNKS = 4


def nt_dot(lhs, rhs):
    return lax.dot_general(lhs, rhs, (((1,), (1,)), ((), ())), preferred_element_type=F32)


def kernel(
    state, right, left, coup, term, outc, dims,
    out_ref,
    ring, mbuf, mfull, lbuf, cbuf, xbuf, part, acc2, acc3, acc4, inbox, mid, inmid, last, inlast,
    vcoup, vterm, vout, sdims,
    local_sem, s_send, s_recv, r_send, r_recv, pair_send, pair_recv,
    x_send, x_recv, a_send, a_recv, m_send, m_recv, b_send, b_recv,
):
    sectors = lax.axis_size("sec")
    panels = lax.axis_size("pan")
    ring_size = panels // 2
    terms, cols, width = right.shape
    channels, rows, _ = left.shape
    sec = lax.axis_index("sec")
    pan = lax.axis_index("pan")
    zed = pan // 2
    core = lax.rem(pan, 2)
    partner = pan + 1 - 2 * core
    ahead = lax.rem(pan + 2, panels)
    behind = lax.rem(pan + panels - 2, panels)
    half = rows // 2
    per_chunk = terms // CHUNKS
    per_last = terms // 2 // LAST_CHUNKS

    def sector_at(offset):
        return lax.rem(sec + offset + sectors, sectors)

    def has_sector(offset):
        return (sec + offset >= 0) & (sec + offset < sectors)

    copy_right = pltpu.make_async_copy(right, ring.at[0], local_sem.at[0])
    copy_state = pltpu.make_async_copy(state.at[0], mbuf.at[pan], local_sem.at[1])
    copy_left = [
        pltpu.make_async_copy(left.at[:, pl.ds(g * half, half), :], lbuf.at[g], local_sem.at[2])
        for g in range(2)
    ]
    tables = [
        pltpu.make_async_copy(coup, vcoup, local_sem.at[3]),
        pltpu.make_async_copy(term, vterm, local_sem.at[4]),
        pltpu.make_async_copy(outc, vout, local_sem.at[5]),
        pltpu.make_async_copy(dims, sdims, local_sem.at[6]),
    ]
    barrier = pltpu.get_barrier_semaphore()
    for peer in (ahead, behind, partner):
        pl.semaphore_signal(barrier, inc=1, device_id=(sec, peer), device_id_type=MESH)
    greeted = 3
    for offset in OFFSETS:
        exists = has_sector(offset)
        greeted = greeted + 2 * jnp.where(exists, 1, 0)

        @pl.when(exists)
        def _():
            for other in (pan, partner):
                pl.semaphore_signal(
                    barrier, inc=1, device_id=(sector_at(offset), other), device_id_type=MESH
                )

    copy_state.start()
    copy_right.start()
    for copy in tables:
        copy.start()
    for copy in copy_left:
        copy.start()

    with jax.named_scope("barrier"):
        pl.semaphore_wait(barrier, greeted)

    for offset in OFFSETS:

        @pl.when(jnp.logical_not(has_sector(-offset)))
        def _():
            inbox[offset + 2] = jnp.zeros(inbox.shape[1:], F32)
            inmid[offset + 2] = jnp.zeros(inmid.shape[1:], F32)
            inlast[offset + 2] = jnp.zeros(inlast.shape[1:], F32)

    def state_hop(way, dist, part_rows, index):
        sign = 1 if way == 0 else -1
        owner = lax.rem(pan - sign * 2 * (dist - 1) + panels, panels)
        return pltpu.make_async_remote_copy(
            src_ref=mbuf.at[owner, part_rows],
            dst_ref=mbuf.at[owner, part_rows],
            send_sem=s_send.at[way],
            recv_sem=s_recv.at[way, index],
            device_id=(sec, ahead if way == 0 else behind),
            device_id_type=MESH,
        )

    def state_arrival(way, dist, part_rows, index):
        sign = 1 if way == 0 else -1
        owner = lax.rem(pan - sign * 2 * dist + 2 * panels, panels)
        return pltpu.make_async_remote_copy(
            src_ref=mbuf.at[owner, part_rows],
            dst_ref=mbuf.at[owner, part_rows],
            send_sem=s_send.at[way],
            recv_sem=s_recv.at[way, index],
            device_id=(sec, ahead if way == 0 else behind),
            device_id_type=MESH,
        )

    def state_rows(way, dist):
        if dist < 4:
            return pl.ds(0, rows)
        return pl.ds(way * half, half)

    def slot(way, dist):
        if dist == 0:
            return 0
        return ring_size - dist if way == 0 else dist

    def ring_hop(way, dist, chunk):
        if dist < 4:
            piece = pl.ds(chunk * per_chunk, per_chunk)
        else:
            piece = pl.ds(way * (terms // 2) + chunk * per_last, per_last)
        return pltpu.make_async_remote_copy(
            src_ref=ring.at[slot(way, dist - 1), piece],
            dst_ref=ring.at[slot(way, dist), piece],
            send_sem=r_send.at[way],
            recv_sem=r_recv.at[way, (dist - 1) * CHUNKS + chunk],
            device_id=(sec, ahead if way == 0 else behind),
            device_id_type=MESH,
        )

    def send_state(dist):
        for way in range(2):
            state_hop(way, dist, state_rows(way, dist), dist - 1).start()

    def wait_state(dist):
        for way in range(2):
            state_arrival(way, dist, state_rows(way, dist), dist - 1).wait_recv()

    def send_own(chunk):
        for way in range(2):
            ring_hop(way, 1, chunk).start()

    def service(dist, chunk):
        for way in range(2):
            ring_hop(way, dist, chunk).wait_recv()
            if dist < 3:
                ring_hop(way, dist + 1, chunk).start()
            else:
                for piece in range(LAST_CHUNKS):
                    first = way * (terms // 2) + piece * per_last
                    if first // per_chunk == chunk:
                        ring_hop(way, 4, piece).start()

    with jax.named_scope("own_state"):
        copy_state.wait()
        send_state(1)
    with jax.named_scope("own_right"):
        copy_right.wait()
        send_own(0)

    for copy in tables:
        copy.wait()
    live = sdims[0, 0]
    lanes = channels * half
    slot_row = (vout[...] - sec + 2).astype(F32)
    table = jnp.concatenate(
        [slot_row, vterm[...].astype(F32), vcoup[...].astype(F32), jnp.zeros((5, channels), F32)], axis=0
    ).astype(BF16)
    chan_of_lane = lax.broadcasted_iota(jnp.int32, (channels, lanes), 1) // half
    chan = lax.broadcasted_iota(jnp.int32, (channels, lanes), 0)
    spread = jnp.where(chan_of_lane == chan, 1.0, 0.0).astype(BF16)
    wide = jnp.dot(table, spread, preferred_element_type=F32)
    row_in_half = lax.rem(lax.broadcasted_iota(jnp.int32, (1, lanes), 1), half).astype(F32)
    target = (wide[1:2] * 5.0 + wide[0:1]) * float(half) + row_in_half
    weight = wide[2:3]

    tile = 256

    def combine(step):
        at = lax.broadcasted_iota(jnp.int32, (tile, lanes), 0).astype(F32) + float(step * tile)
        kron = jnp.where(at == target, weight, 0.0).astype(BF16)
        for g in range(2):
            made = jnp.dot(kron, lbuf[g].reshape(lanes, width), preferred_element_type=F32).astype(BF16)
            groups = tile // half
            cbuf[pl.ds(step * groups, groups), g] = made.reshape(groups, half, width)

    pltpu.make_async_copy(lbuf, lbuf, local_sem.at[2]).wait()
    with jax.named_scope("combine_a"):
        combine(0)
        combine(1)
    with jax.named_scope("hop_1"):
        wait_state(1)
    send_state(2)
    send_own(1)
    combine(2)
    combine(3)
    with jax.named_scope("hop_2"):
        wait_state(2)
    send_state(3)
    send_own(2)
    combine(4)
    with jax.named_scope("hop_3"):
        wait_state(3)
    send_state(4)
    send_own(3)
    service(1, 0)
    with jax.named_scope("hop_4"):
        wait_state(4)
    def pair_copy(step):
        return pltpu.make_async_remote_copy(
            src_ref=mbuf.at[2 * step + core],
            dst_ref=mbuf.at[2 * step + core],
            send_sem=pair_send,
            recv_sem=pair_recv,
            device_id=(sec, partner),
            device_id_type=MESH,
        )

    for step in range(ring_size):
        pair_copy(step).start()
    service(1, 1)
    pair_all = pltpu.make_async_remote_copy(
        src_ref=mbuf.at[pl.ds(0, ring_size)],
        dst_ref=mbuf.at[pl.ds(0, ring_size)],
        send_sem=pair_send,
        recv_sem=pair_recv,
        device_id=(sec, partner),
        device_id_type=MESH,
    )
    pair_all.wait_recv()

    row_at = lax.broadcasted_iota(jnp.int32, (width, width), 0)
    col_at = lax.broadcasted_iota(jnp.int32, (width, width), 1)
    masked = jnp.where(
        (row_at < live) & (col_at < live), mbuf[...].reshape(width, width), jnp.zeros((), BF16)
    )
    mfull[...] = masked
    group = 4
    for step in range(terms // group):
        block = cbuf[pl.ds(step * group * 5, group * 5)].reshape(group * 5 * rows, width)
        made = jnp.dot(block, mfull[...], preferred_element_type=F32).astype(BF16)
        xbuf[pl.ds(step * group, group), core] = made.reshape(group, 5 * rows, width)
        if step % 2:
            service(1, 2 + step // 2)
        pltpu.make_async_remote_copy(
            src_ref=xbuf.at[pl.ds(step * group, group), core],
            dst_ref=xbuf.at[pl.ds(step * group, group), core],
            send_sem=x_send,
            recv_sem=x_recv,
            device_id=(sec, partner),
            device_id_type=MESH,
        ).start()
    x_all = pltpu.make_async_remote_copy(
        src_ref=xbuf.at[:, core],
        dst_ref=xbuf.at[:, core],
        send_sem=x_send,
        recv_sem=x_recv,
        device_id=(sec, partner),
        device_id_type=MESH,
    )

    part[...] = jnp.zeros(part.shape, F32)
    x_all.wait_recv()

    def contract(slots, which, held):
        blocks = []
        for w in which:
            pieces = [ring[k, w] for k in slots]
            blocks.append(pieces[0] if len(pieces) == 1 else jnp.concatenate(pieces, axis=0))
        totals = []
        for owner in range(2):
            total = None if held is None else held[owner]
            for w, block in zip(which, blocks):
                product = nt_dot(xbuf[w, owner], block)
                total = product if total is None else total + product
            totals.append(total)
        return totals

    def place(slots, totals):
        for owner, total in enumerate(totals):
            for i, k in enumerate(slots):
                piece = total[:, i * cols : (i + 1) * cols].reshape(5, rows, cols)
                part[pl.ds(owner * 5, 5), :, pl.ds(k * cols, cols)] = piece

    def keep_in(acc, totals):
        for owner, total in enumerate(totals):
            acc[owner] = total

    def pack(total):
        total = total.reshape(5, rows // 8, 8, cols)
        return jnp.concatenate([total[:, i] for i in range(rows // 8)], axis=2)

    def unpack(packed):
        return jnp.concatenate([packed[:, i * cols : (i + 1) * cols] for i in range(rows // 8)], axis=0)

    def exchange(source, landing, send_sem, recv_sem):
        def copy_to(which, j):
            return pltpu.make_async_remote_copy(
                src_ref=source.at[which * 5 + j],
                dst_ref=landing.at[j, core],
                send_sem=send_sem.at[j],
                recv_sem=recv_sem.at[j],
                device_id=(sector_at(j - 2), 2 * zed + which),
                device_id_type=MESH,
            )

        def both(j):
            return pltpu.make_async_remote_copy(
                src_ref=source.at[pl.ds(0, 2)],
                dst_ref=landing.at[j],
                send_sem=send_sem.at[j],
                recv_sem=recv_sem.at[j],
                device_id=(sec, partner),
                device_id_type=MESH,
            )

        def start():
            for j in (0, 4, 1, 3):

                @pl.when(has_sector(j - 2))
                def _():
                    for which in range(2):
                        copy_to(which, j).start()

            copy_to(1 - core, 2).start()

        def wait_recv():
            for j in (0, 4, 1, 3):

                @pl.when(has_sector(2 - j))
                def _():
                    both(j).wait_recv()

            copy_to(1 - core, 2).wait_recv()

        def wait_send():
            for j in (0, 4, 1, 3):

                @pl.when(has_sector(j - 2))
                def _():
                    both(j).wait_send()

            copy_to(1 - core, 2).wait_send()

        return start, wait_recv, wait_send

    def sum_of(landing, cls):
        total = landing[0, cls]
        for j in range(1, 5):
            total = total + landing[j, cls]
        return total

    start_a, recv_a, sent_a = exchange(part, inbox, a_send, a_recv)
    start_m, recv_m, sent_m = exchange(mid, inmid, m_send, m_recv)
    start_b, recv_b, sent_b = exchange(last, inlast, b_send, b_recv)

    def chunk_terms(chunk):
        return range(chunk * per_chunk, (chunk + 1) * per_chunk)

    with jax.named_scope("contract_a"):
        place((0, 1, 7), contract((0, 1, 7), range(terms), None))
    with jax.named_scope("ring_2"):
        for chunk in range(CHUNKS):
            service(2, chunk)
            totals = contract((2, 6), chunk_terms(chunk), acc2 if chunk else None)
            if chunk < CHUNKS - 1:
                keep_in(acc2, totals)
            else:
                place((2, 6), totals)
    with jax.named_scope("ring_3"):
        for chunk in range(CHUNKS):
            service(3, chunk)
            if chunk == 0:
                start_a()
            keep_in(acc3, contract((3, 5), chunk_terms(chunk), acc3 if chunk else None))
        for owner in range(2):
            for i in range(2):
                mid[pl.ds(owner * 5, 5), pl.ds(8 * i, 8)] = pack(acc3[owner, :, pl.ds(i * cols, cols)])

    def by_final_step(step):
        low = list(range(step * per_last, (step + 1) * per_last))
        return low + [terms // 2 + w for w in low]

    def final_wait(step):
        for way in range(2):
            ring_hop(way, 4, step).wait_recv()

    final_wait(0)
    start_m()
    keep_in(acc4, contract((4,), by_final_step(0), None))
    for step in range(1, LAST_CHUNKS - 1):
        final_wait(step)
        keep_in(acc4, contract((4,), by_final_step(step), acc4))
    with jax.named_scope("final_wait"):
        final_wait(LAST_CHUNKS - 1)
    with jax.named_scope("last"):
        totals = contract((4,), by_final_step(LAST_CHUNKS - 1), acc4)
        for owner in range(2):
            last[pl.ds(owner * 5, 5)] = pack(totals[owner])
        start_b()

    recv_a()
    inbox[2, core] = part[core * 5 + 2]
    inmid[2, core] = mid[core * 5 + 2]
    inlast[2, core] = last[core * 5 + 2]
    recv_m()
    sums = []
    for cls in range(2):
        total = sum_of(inbox, cls)
        extra = sum_of(inmid, cls)
        total = jnp.concatenate(
            [
                total[:, : 3 * cols],
                unpack(extra[:8]),
                total[:, 4 * cols : 5 * cols],
                unpack(extra[8:]),
                total[:, 6 * cols :],
            ],
            axis=1,
        )
        sums.append(pltpu.roll(total, zed * cols, axis=1))
    pieces = []
    for k in range(ring_size):
        for cls in range(2):
            pieces.append(sums[cls][:, k * cols : (k + 1) * cols])
    early = jnp.concatenate(pieces, axis=1)
    lane = lax.broadcasted_iota(jnp.int32, (rows, width), 1)
    here = lane // (2 * cols) == lax.rem(zed + 4, ring_size)
    with jax.named_scope("sent"):
        for way in range(2):
            pltpu.make_async_remote_copy(
                src_ref=mbuf.at[pl.ds(0, 7), pl.ds(0, half)],
                dst_ref=mbuf.at[pl.ds(0, 7), pl.ds(0, half)],
                send_sem=s_send.at[way],
                recv_sem=s_recv.at[way, 0],
                device_id=(sec, partner),
                device_id_type=MESH,
            ).wait_send()
            pltpu.make_async_remote_copy(
                src_ref=ring.at[pl.ds(0, 7), pl.ds(0, terms // 2)],
                dst_ref=ring.at[pl.ds(0, 7), pl.ds(0, terms // 2)],
                send_sem=r_send.at[way],
                recv_sem=r_recv.at[way, 0],
                device_id=(sec, partner),
                device_id_type=MESH,
            ).wait_send()
        pair_all.wait_send()
        x_all.wait_send()
        sent_a()
        sent_m()
        sent_b()
    with jax.named_scope("recv_b"):
        recv_b()
    with jax.named_scope("finish"):
        lasts = [unpack(sum_of(inlast, cls)) for cls in range(2)]
        late = jnp.concatenate(lasts * (width // (2 * cols)), axis=1)
        out_ref[0] = early + jnp.where(here, late, 0.0)


def on_device(
    wave_state, right_blocks, left_blocks, coupling, channel_term, channel_out, sector_dims
):
    _, rows, width = wave_state.shape
    _, terms, _, cols = right_blocks.shape
    channels = left_blocks.shape[0]
    panels = lax.axis_size("pan")
    ring_size = panels // 2
    half = rows // 2
    right = jnp.swapaxes(right_blocks[0], 1, 2)
    dma = pltpu.SemaphoreType.DMA
    applied = pl.pallas_call(
        kernel,
        out_shape=jax.ShapeDtypeStruct((1, rows, width), F32),
        in_specs=[pl.BlockSpec(memory_space=pltpu.HBM)] * 7,
        out_specs=pl.BlockSpec(memory_space=pltpu.VMEM),
        scratch_shapes=[
            pltpu.VMEM((ring_size, terms, cols, width), BF16),
            pltpu.VMEM((panels, rows, width), BF16),
            pltpu.VMEM((width, width), BF16),
            pltpu.VMEM((2, channels, half, width), BF16),
            pltpu.VMEM((5 * terms, 2, half, width), BF16),
            pltpu.VMEM((terms, 2, 5 * rows, width), BF16),
            pltpu.VMEM((10, rows, ring_size * cols), F32),
            pltpu.VMEM((2, 5 * rows, 2 * cols), F32),
            pltpu.VMEM((2, 5 * rows, 2 * cols), F32),
            pltpu.VMEM((2, 5 * rows, cols), F32),
            pltpu.VMEM((5, 2, rows, ring_size * cols), F32),
            pltpu.VMEM((10, 16, rows // 8 * cols), F32),
            pltpu.VMEM((5, 2, 16, rows // 8 * cols), F32),
            pltpu.VMEM((10, 8, rows // 8 * cols), F32),
            pltpu.VMEM((5, 2, 8, rows // 8 * cols), F32),
            pltpu.VMEM((1, channels), BF16),
            pltpu.VMEM((1, channels), jnp.int32),
            pltpu.VMEM((1, channels), jnp.int32),
            pltpu.SMEM((1, 1), jnp.int32),
            dma((7,)),
            dma((2,)),
            dma((2, 4)),
            dma((2,)),
            dma((2, 3 * CHUNKS + LAST_CHUNKS)),
            dma(()),
            dma(()),
            dma(()),
            dma(()),
            dma((5,)),
            dma((5,)),
            dma((5,)),
            dma((5,)),
            dma((5,)),
            dma((5,)),
        ],
        compiler_params=pltpu.CompilerParams(
            collective_id=0, has_side_effects=True, vmem_limit_bytes=60 * 1024 * 1024
        ),
        name="sector_step",
    )(
        wave_state,
        right,
        left_blocks,
        coupling[None],
        channel_term[None],
        channel_out[None],
        sector_dims[None],
    )
    live = sector_dims[0]
    row_ids = lax.axis_index("pan") * rows + lax.iota(jnp.int32, rows)
    kept_mask = (row_ids[:, None] < live) & (lax.iota(jnp.int32, width)[None, :] < live)
    return jnp.where(kept_mask[None], applied, jnp.zeros((), F32))


def solution(mesh):
    return jax.shard_map(
        on_device,
        mesh=mesh,
        in_specs=(
            P("sec", "pan", None),
            P("sec", None, None, "pan"),
            P("sec", "pan", None),
            P("sec"),
            P("sec"),
            P("sec"),
            P("sec"),
        ),
        out_specs=P("sec", "pan", None),
        check_vma=False,
    )
```

```python
import jax
import jax.numpy as jnp
from jax import lax
from jax.experimental import pallas as pl
from jax.experimental.pallas import tpu as pltpu
from jax.sharding import PartitionSpec as P

MESH = pl.DeviceIdType.MESH
F32 = jnp.float32
BF16 = jnp.bfloat16
OFFSETS = (-2, -1, 1, 2)
CHUNKS = 4
LAST_TERMS = (3, 2, 2, 1)
LAST_CHUNKS = len(LAST_TERMS)


def nt_dot(lhs, rhs):
    return lax.dot_general(lhs, rhs, (((1,), (1,)), ((), ())), preferred_element_type=F32)


def kernel(
    state, right, left, coup, term, outc, dims,
    out_ref,
    ring, mbuf, mfull, lbuf, cbuf, xbuf, part, acc2, acc3, acc4, inbox, mid, inmid, last, inlast,
    vcoup, vterm, vout, sdims,
    local_sem, s_send, s_recv, r_send, r_recv, pair_send, pair_recv,
    x_send, x_recv, a_send, a_recv, m_send, m_recv, b_send, b_recv, column_sem, ready_sem,
):
    sectors = lax.axis_size("sec")
    panels = lax.axis_size("pan")
    ring_size = panels // 2
    terms, cols, width = right.shape
    channels, rows, _ = left.shape
    sec = lax.axis_index("sec")
    pan = lax.axis_index("pan")
    zed = pan // 2
    core = lax.rem(pan, 2)
    partner = pan + 1 - 2 * core
    ahead = lax.rem(pan + 2, panels)
    behind = lax.rem(pan + panels - 2, panels)
    half = rows // 2
    per_chunk = terms // CHUNKS
    last_from = [sum(LAST_TERMS[:i]) for i in range(LAST_CHUNKS)]

    def sector_at(offset):
        return lax.rem(sec + offset + sectors, sectors)

    def has_sector(offset):
        return (sec + offset >= 0) & (sec + offset < sectors)

    copy_right = pltpu.make_async_copy(right, ring.at[0], local_sem.at[0])
    copy_state = pltpu.make_async_copy(state.at[0], mbuf.at[pan], local_sem.at[1])
    copy_left = [
        pltpu.make_async_copy(left.at[:, pl.ds(g * half, half), :], lbuf.at[g], local_sem.at[2])
        for g in range(2)
    ]
    tables = [
        pltpu.make_async_copy(coup, vcoup, local_sem.at[3]),
        pltpu.make_async_copy(term, vterm, local_sem.at[4]),
        pltpu.make_async_copy(outc, vout, local_sem.at[5]),
        pltpu.make_async_copy(dims, sdims, local_sem.at[6]),
    ]
    barrier = pltpu.get_barrier_semaphore()
    first = zed == 0
    for peer in (ahead, behind, partner):
        pl.semaphore_signal(barrier, inc=1, device_id=(sec, peer), device_id_type=MESH)
    others = 0
    for offset in OFFSETS:
        exists = has_sector(offset)
        others = others + 2 * jnp.where(exists, 1, 0)

        @pl.when(first & exists)
        def _():
            for other in (pan, partner):
                pl.semaphore_signal(
                    barrier, inc=1, device_id=(sector_at(offset), other), device_id_type=MESH
                )

    copy_state.start()
    copy_right.start()
    for copy in tables:
        copy.start()
    for copy in copy_left:
        copy.start()

    with jax.named_scope("barrier"):
        pl.semaphore_wait(barrier, 3 + jnp.where(first, others, 0))

    for offset in OFFSETS:

        @pl.when(jnp.logical_not(has_sector(-offset)))
        def _():
            inbox[offset + 2] = jnp.zeros(inbox.shape[1:], F32)
            inmid[offset + 2] = jnp.zeros(inmid.shape[1:], F32)
            inlast[offset + 2] = jnp.zeros(inlast.shape[1:], F32)

    def state_hop(way, dist, part_rows, index):
        sign = 1 if way == 0 else -1
        owner = lax.rem(pan - sign * 2 * (dist - 1) + panels, panels)
        return pltpu.make_async_remote_copy(
            src_ref=mbuf.at[owner, part_rows],
            dst_ref=mbuf.at[owner, part_rows],
            send_sem=s_send.at[way],
            recv_sem=s_recv.at[way, index],
            device_id=(sec, ahead if way == 0 else behind),
            device_id_type=MESH,
        )

    def state_arrival(way, dist, part_rows, index):
        sign = 1 if way == 0 else -1
        owner = lax.rem(pan - sign * 2 * dist + 2 * panels, panels)
        return pltpu.make_async_remote_copy(
            src_ref=mbuf.at[owner, part_rows],
            dst_ref=mbuf.at[owner, part_rows],
            send_sem=s_send.at[way],
            recv_sem=s_recv.at[way, index],
            device_id=(sec, ahead if way == 0 else behind),
            device_id_type=MESH,
        )

    def state_rows(way, dist):
        if dist < 4:
            return pl.ds(0, rows)
        return pl.ds(way * half, half)

    def slot(way, dist):
        if dist == 0:
            return 0
        return ring_size - dist if way == 0 else dist

    def ring_hop(way, dist, chunk):
        if dist < 4:
            piece = pl.ds(chunk * per_chunk, per_chunk)
        else:
            piece = pl.ds(way * (terms // 2) + last_from[chunk], LAST_TERMS[chunk])
        return pltpu.make_async_remote_copy(
            src_ref=ring.at[slot(way, dist - 1), piece],
            dst_ref=ring.at[slot(way, dist), piece],
            send_sem=r_send.at[way],
            recv_sem=r_recv.at[way, (dist - 1) * CHUNKS + chunk],
            device_id=(sec, ahead if way == 0 else behind),
            device_id_type=MESH,
        )

    def send_state(dist):
        for way in range(2):
            state_hop(way, dist, state_rows(way, dist), dist - 1).start()

    def wait_state(dist):
        for way in range(2):
            state_arrival(way, dist, state_rows(way, dist), dist - 1).wait_recv()

    def send_own(chunk):
        for way in range(2):
            ring_hop(way, 1, chunk).start()

    def service(dist, chunk):
        for way in range(2):
            ring_hop(way, dist, chunk).wait_recv()
            if dist < 3:
                ring_hop(way, dist + 1, chunk).start()
            else:
                for piece in range(LAST_CHUNKS):
                    end = way * (terms // 2) + last_from[piece] + LAST_TERMS[piece]
                    if (end - 1) // per_chunk == chunk:
                        ring_hop(way, 4, piece).start()

    with jax.named_scope("own_state"):
        copy_state.wait()
        send_state(1)
    with jax.named_scope("own_right"):
        copy_right.wait()
        send_own(0)

    for copy in tables:
        copy.wait()
    live = sdims[0, 0]
    lanes = channels * half
    slot_row = (vout[...] - sec + 2).astype(F32)
    table = jnp.concatenate(
        [slot_row, vterm[...].astype(F32), vcoup[...].astype(F32), jnp.zeros((5, channels), F32)], axis=0
    ).astype(BF16)
    chan_of_lane = lax.broadcasted_iota(jnp.int32, (channels, lanes), 1) // half
    chan = lax.broadcasted_iota(jnp.int32, (channels, lanes), 0)
    spread = jnp.where(chan_of_lane == chan, 1.0, 0.0).astype(BF16)
    wide = jnp.dot(table, spread, preferred_element_type=F32)
    row_in_half = lax.rem(lax.broadcasted_iota(jnp.int32, (1, lanes), 1), half).astype(F32)
    target = (wide[1:2] * 5.0 + wide[0:1]) * float(half) + row_in_half
    weight = wide[2:3]

    tile = 256

    def combine(step):
        at = lax.broadcasted_iota(jnp.int32, (tile, lanes), 0).astype(F32) + float(step * tile)
        kron = jnp.where(at == target, weight, 0.0).astype(BF16)
        for g in range(2):
            made = jnp.dot(kron, lbuf[g].reshape(lanes, width), preferred_element_type=F32).astype(BF16)
            groups = tile // half
            cbuf[pl.ds(step * groups, groups), g] = made.reshape(groups, half, width)

    pltpu.make_async_copy(lbuf, lbuf, local_sem.at[2]).wait()
    with jax.named_scope("combine_a"):
        combine(0)
        combine(1)
    with jax.named_scope("hop_1"):
        wait_state(1)
    send_state(2)
    send_own(1)
    combine(2)
    combine(3)
    with jax.named_scope("hop_2"):
        wait_state(2)
    send_state(3)
    send_own(2)
    combine(4)
    with jax.named_scope("hop_3"):
        wait_state(3)
    send_state(4)
    send_own(3)
    service(1, 0)
    with jax.named_scope("hop_4"):
        wait_state(4)
    def pair_copy(step):
        return pltpu.make_async_remote_copy(
            src_ref=mbuf.at[2 * step + core],
            dst_ref=mbuf.at[2 * step + core],
            send_sem=pair_send,
            recv_sem=pair_recv,
            device_id=(sec, partner),
            device_id_type=MESH,
        )

    for step in range(ring_size):
        pair_copy(step).start()
    for offset in OFFSETS:

        @pl.when(first & has_sector(offset))
        def _():
            for other in (pan, partner):
                pl.semaphore_signal(
                    column_sem, inc=1, device_id=(sector_at(offset), other), device_id_type=MESH
                )

    service(1, 1)
    pair_all = pltpu.make_async_remote_copy(
        src_ref=mbuf.at[pl.ds(0, ring_size)],
        dst_ref=mbuf.at[pl.ds(0, ring_size)],
        send_sem=pair_send,
        recv_sem=pair_recv,
        device_id=(sec, partner),
        device_id_type=MESH,
    )
    pair_all.wait_recv()

    row_at = lax.broadcasted_iota(jnp.int32, (width, width), 0)
    col_at = lax.broadcasted_iota(jnp.int32, (width, width), 1)
    masked = jnp.where(
        (row_at < live) & (col_at < live), mbuf[...].reshape(width, width), jnp.zeros((), BF16)
    )
    mfull[...] = masked
    group = 4
    for step in range(terms // group):
        block = cbuf[pl.ds(step * group * 5, group * 5)].reshape(group * 5 * rows, width)
        made = jnp.dot(block, mfull[...], preferred_element_type=F32).astype(BF16)
        xbuf[pl.ds(step * group, group), core] = made.reshape(group, 5 * rows, width)
        if step % 2:
            service(1, 2 + step // 2)
        pltpu.make_async_remote_copy(
            src_ref=xbuf.at[pl.ds(step * group, group), core],
            dst_ref=xbuf.at[pl.ds(step * group, group), core],
            send_sem=x_send,
            recv_sem=x_recv,
            device_id=(sec, partner),
            device_id_type=MESH,
        ).start()
    x_all = pltpu.make_async_remote_copy(
        src_ref=xbuf.at[:, core],
        dst_ref=xbuf.at[:, core],
        send_sem=x_send,
        recv_sem=x_recv,
        device_id=(sec, partner),
        device_id_type=MESH,
    )

    @pl.when(first)
    def _():
        pl.semaphore_wait(column_sem, others)
        for step in range(1, ring_size):
            pl.semaphore_signal(
                ready_sem, inc=1, device_id=(sec, 2 * step + core), device_id_type=MESH
            )

    part[...] = jnp.zeros(part.shape, F32)
    x_all.wait_recv()

    def contract(slots, which, held):
        blocks = []
        for w in which:
            pieces = [ring[k, w] for k in slots]
            blocks.append(pieces[0] if len(pieces) == 1 else jnp.concatenate(pieces, axis=0))
        totals = []
        for owner in range(2):
            total = None if held is None else held[owner]
            for w, block in zip(which, blocks):
                product = nt_dot(xbuf[w, owner], block)
                total = product if total is None else total + product
            totals.append(total)
        return totals

    def place(slots, totals):
        for owner, total in enumerate(totals):
            for i, k in enumerate(slots):
                piece = total[:, i * cols : (i + 1) * cols].reshape(5, rows, cols)
                part[pl.ds(owner * 5, 5), :, pl.ds(k * cols, cols)] = piece

    def keep_in(acc, totals):
        for owner, total in enumerate(totals):
            acc[owner] = total

    def pack(total):
        total = total.reshape(5, rows // 8, 8, cols)
        return jnp.concatenate([total[:, i] for i in range(rows // 8)], axis=2)

    def unpack(packed):
        return jnp.concatenate([packed[:, i * cols : (i + 1) * cols] for i in range(rows // 8)], axis=0)

    def exchange(source, landing, send_sem, recv_sem):
        def copy_to(which, j):
            return pltpu.make_async_remote_copy(
                src_ref=source.at[which * 5 + j],
                dst_ref=landing.at[j, core],
                send_sem=send_sem.at[j],
                recv_sem=recv_sem.at[j],
                device_id=(sector_at(j - 2), 2 * zed + which),
                device_id_type=MESH,
            )

        def both(j):
            return pltpu.make_async_remote_copy(
                src_ref=source.at[pl.ds(0, 2)],
                dst_ref=landing.at[j],
                send_sem=send_sem.at[j],
                recv_sem=recv_sem.at[j],
                device_id=(sec, partner),
                device_id_type=MESH,
            )

        def start():
            for j in (0, 4, 1, 3):

                @pl.when(has_sector(j - 2))
                def _():
                    for which in range(2):
                        copy_to(which, j).start()

            copy_to(1 - core, 2).start()

        def wait_recv():
            for j in (0, 4, 1, 3):

                @pl.when(has_sector(2 - j))
                def _():
                    both(j).wait_recv()

            copy_to(1 - core, 2).wait_recv()

        def wait_send():
            for j in (0, 4, 1, 3):

                @pl.when(has_sector(j - 2))
                def _():
                    both(j).wait_send()

            copy_to(1 - core, 2).wait_send()

        return start, wait_recv, wait_send

    def sum_of(landing, cls):
        total = landing[0, cls]
        for j in range(1, 5):
            total = total + landing[j, cls]
        return total

    start_a, recv_a, sent_a = exchange(part, inbox, a_send, a_recv)
    start_m, recv_m, sent_m = exchange(mid, inmid, m_send, m_recv)
    start_b, recv_b, sent_b = exchange(last, inlast, b_send, b_recv)

    def chunk_terms(chunk):
        return range(chunk * per_chunk, (chunk + 1) * per_chunk)

    with jax.named_scope("contract_a"):
        place((0, 1, 7), contract((0, 1, 7), range(terms), None))
    with jax.named_scope("ring_2"):
        for chunk in range(CHUNKS):
            service(2, chunk)
            totals = contract((2, 6), chunk_terms(chunk), acc2 if chunk else None)
            if chunk < CHUNKS - 1:
                keep_in(acc2, totals)
            else:
                place((2, 6), totals)
    with jax.named_scope("ring_3"):
        for chunk in range(CHUNKS):
            service(3, chunk)
            if chunk == 0:

                @pl.when(jnp.logical_not(first))
                def _():
                    pl.semaphore_wait(ready_sem, 1)

                start_a()
            keep_in(acc3, contract((3, 5), chunk_terms(chunk), acc3 if chunk else None))
        for owner in range(2):
            for i in range(2):
                mid[pl.ds(owner * 5, 5), pl.ds(8 * i, 8)] = pack(acc3[owner, :, pl.ds(i * cols, cols)])

    def by_final_step(step):
        low = list(range(last_from[step], last_from[step] + LAST_TERMS[step]))
        return low + [terms // 2 + w for w in low]

    def final_wait(step):
        for way in range(2):
            ring_hop(way, 4, step).wait_recv()

    final_wait(0)
    start_m()
    keep_in(acc4, contract((4,), by_final_step(0), None))
    for step in range(1, LAST_CHUNKS - 1):
        final_wait(step)
        keep_in(acc4, contract((4,), by_final_step(step), acc4))
    with jax.named_scope("final_wait"):
        final_wait(LAST_CHUNKS - 1)
    with jax.named_scope("last"):
        totals = contract((4,), by_final_step(LAST_CHUNKS - 1), acc4)
        for owner in range(2):
            last[pl.ds(owner * 5, 5)] = pack(totals[owner])
        start_b()

    recv_a()
    inbox[2, core] = part[core * 5 + 2]
    inmid[2, core] = mid[core * 5 + 2]
    inlast[2, core] = last[core * 5 + 2]
    recv_m()
    sums = []
    for cls in range(2):
        total = sum_of(inbox, cls)
        extra = sum_of(inmid, cls)
        total = jnp.concatenate(
            [
                total[:, : 3 * cols],
                unpack(extra[:8]),
                total[:, 4 * cols : 5 * cols],
                unpack(extra[8:]),
                total[:, 6 * cols :],
            ],
            axis=1,
        )
        sums.append(pltpu.roll(total, zed * cols, axis=1))
    pieces = []
    for k in range(ring_size):
        for cls in range(2):
            pieces.append(sums[cls][:, k * cols : (k + 1) * cols])
    early = jnp.concatenate(pieces, axis=1)
    lane = lax.broadcasted_iota(jnp.int32, (rows, width), 1)
    here = lane // (2 * cols) == lax.rem(zed + 4, ring_size)
    with jax.named_scope("sent"):
        for way in range(2):
            pltpu.make_async_remote_copy(
                src_ref=mbuf.at[pl.ds(0, 7), pl.ds(0, half)],
                dst_ref=mbuf.at[pl.ds(0, 7), pl.ds(0, half)],
                send_sem=s_send.at[way],
                recv_sem=s_recv.at[way, 0],
                device_id=(sec, partner),
                device_id_type=MESH,
            ).wait_send()
            pltpu.make_async_remote_copy(
                src_ref=ring.at[pl.ds(0, 7), pl.ds(0, terms // 2)],
                dst_ref=ring.at[pl.ds(0, 7), pl.ds(0, terms // 2)],
                send_sem=r_send.at[way],
                recv_sem=r_recv.at[way, 0],
                device_id=(sec, partner),
                device_id_type=MESH,
            ).wait_send()
        pair_all.wait_send()
        x_all.wait_send()
        sent_a()
        sent_m()
        sent_b()
    with jax.named_scope("recv_b"):
        recv_b()
    with jax.named_scope("finish"):
        lasts = [unpack(sum_of(inlast, cls)) for cls in range(2)]
        late = jnp.concatenate(lasts * (width // (2 * cols)), axis=1)
        out_ref[0] = early + jnp.where(here, late, 0.0)


def on_device(
    wave_state, right_blocks, left_blocks, coupling, channel_term, channel_out, sector_dims
):
    _, rows, width = wave_state.shape
    _, terms, _, cols = right_blocks.shape
    channels = left_blocks.shape[0]
    panels = lax.axis_size("pan")
    ring_size = panels // 2
    half = rows // 2
    right = jnp.swapaxes(right_blocks[0], 1, 2)
    dma = pltpu.SemaphoreType.DMA
    applied = pl.pallas_call(
        kernel,
        out_shape=jax.ShapeDtypeStruct((1, rows, width), F32),
        in_specs=[pl.BlockSpec(memory_space=pltpu.HBM)] * 7,
        out_specs=pl.BlockSpec(memory_space=pltpu.VMEM),
        scratch_shapes=[
            pltpu.VMEM((ring_size, terms, cols, width), BF16),
            pltpu.VMEM((panels, rows, width), BF16),
            pltpu.VMEM((width, width), BF16),
            pltpu.VMEM((2, channels, half, width), BF16),
            pltpu.VMEM((5 * terms, 2, half, width), BF16),
            pltpu.VMEM((terms, 2, 5 * rows, width), BF16),
            pltpu.VMEM((10, rows, ring_size * cols), F32),
            pltpu.VMEM((2, 5 * rows, 2 * cols), F32),
            pltpu.VMEM((2, 5 * rows, 2 * cols), F32),
            pltpu.VMEM((2, 5 * rows, cols), F32),
            pltpu.VMEM((5, 2, rows, ring_size * cols), F32),
            pltpu.VMEM((10, 16, rows // 8 * cols), F32),
            pltpu.VMEM((5, 2, 16, rows // 8 * cols), F32),
            pltpu.VMEM((10, 8, rows // 8 * cols), F32),
            pltpu.VMEM((5, 2, 8, rows // 8 * cols), F32),
            pltpu.VMEM((1, channels), BF16),
            pltpu.VMEM((1, channels), jnp.int32),
            pltpu.VMEM((1, channels), jnp.int32),
            pltpu.SMEM((1, 1), jnp.int32),
            dma((7,)),
            dma((2,)),
            dma((2, 4)),
            dma((2,)),
            dma((2, 3 * CHUNKS + LAST_CHUNKS)),
            dma(()),
            dma(()),
            dma(()),
            dma(()),
            dma((5,)),
            dma((5,)),
            dma((5,)),
            dma((5,)),
            dma((5,)),
            dma((5,)),
            pltpu.SemaphoreType.REGULAR,
            pltpu.SemaphoreType.REGULAR,
        ],
        compiler_params=pltpu.CompilerParams(
            collective_id=0, has_side_effects=True, vmem_limit_bytes=60 * 1024 * 1024
        ),
        name="sector_step",
    )(
        wave_state,
        right,
        left_blocks,
        coupling[None],
        channel_term[None],
        channel_out[None],
        sector_dims[None],
    )
    live = sector_dims[0]
    row_ids = lax.axis_index("pan") * rows + lax.iota(jnp.int32, rows)
    kept_mask = (row_ids[:, None] < live) & (lax.iota(jnp.int32, width)[None, :] < live)
    return jnp.where(kept_mask[None], applied, jnp.zeros((), F32))


def solution(mesh):
    return jax.shard_map(
        on_device,
        mesh=mesh,
        in_specs=(
            P("sec", "pan", None),
            P("sec", None, None, "pan"),
            P("sec", "pan", None),
            P("sec"),
            P("sec"),
            P("sec"),
            P("sec"),
        ),
        out_specs=P("sec", "pan", None),
        check_vma=False,
    )
```

```python
import jax
import jax.numpy as jnp
from jax import lax
from jax.experimental import pallas as pl
from jax.experimental.pallas import tpu as pltpu
from jax.sharding import PartitionSpec as P

MESH = pl.DeviceIdType.MESH
F32 = jnp.float32
BF16 = jnp.bfloat16
OFFSETS = (-2, -1, 1, 2)
CHUNKS = 4
LAST_TERMS = (3, 2, 2, 1, 3, 2, 2, 1)
PIECES = len(LAST_TERMS)
EARLY = 1
EARLY_PIECES = 3


def nt_dot(lhs, rhs):
    return lax.dot_general(lhs, rhs, (((1,), (1,)), ((), ())), preferred_element_type=F32)


def kernel(
    state, right, left, coup, term, outc, dims,
    out_ref,
    ring, mbuf, mfull, lbuf, cbuf, xbuf, part, acc2, acc3, acc4, inbox, mid, inmid, last, inlast,
    vcoup, vterm, vout, sdims,
    local_sem, s_send, s_recv, r_send, r_recv, l_send, l_recv, pair_send, pair_recv,
    x_send, x_recv, a_send, a_recv, m_send, m_recv, b_send, b_recv, column_sem, ready_sem,
):
    sectors = lax.axis_size("sec")
    panels = lax.axis_size("pan")
    ring_size = panels // 2
    terms, cols, width = right.shape
    channels, rows, _ = left.shape
    sec = lax.axis_index("sec")
    pan = lax.axis_index("pan")
    zed = pan // 2
    core = lax.rem(pan, 2)
    partner = pan + 1 - 2 * core
    ahead = lax.rem(pan + 2, panels)
    behind = lax.rem(pan + panels - 2, panels)
    half = rows // 2
    per_chunk = terms // CHUNKS
    last_from = [sum(LAST_TERMS[:i]) for i in range(PIECES)]

    def sector_at(offset):
        return lax.rem(sec + offset + sectors, sectors)

    def has_sector(offset):
        return (sec + offset >= 0) & (sec + offset < sectors)

    copy_right = pltpu.make_async_copy(right, ring.at[0], local_sem.at[0])
    copy_state = pltpu.make_async_copy(state.at[0], mbuf.at[pan], local_sem.at[1])
    copy_left = [
        pltpu.make_async_copy(left.at[:, pl.ds(g * half, half), :], lbuf.at[g], local_sem.at[2])
        for g in range(2)
    ]
    tables = [
        pltpu.make_async_copy(coup, vcoup, local_sem.at[3]),
        pltpu.make_async_copy(term, vterm, local_sem.at[4]),
        pltpu.make_async_copy(outc, vout, local_sem.at[5]),
        pltpu.make_async_copy(dims, sdims, local_sem.at[6]),
    ]
    barrier = pltpu.get_barrier_semaphore()
    first = zed == 0
    for peer in (ahead, behind, partner):
        pl.semaphore_signal(barrier, inc=1, device_id=(sec, peer), device_id_type=MESH)
    others = 0
    for offset in OFFSETS:
        exists = has_sector(offset)
        others = others + 2 * jnp.where(exists, 1, 0)

        @pl.when(first & exists)
        def _():
            for other in (pan, partner):
                pl.semaphore_signal(
                    barrier, inc=1, device_id=(sector_at(offset), other), device_id_type=MESH
                )

    copy_state.start()
    copy_right.start()
    for copy in tables:
        copy.start()
    for copy in copy_left:
        copy.start()

    with jax.named_scope("barrier"):
        pl.semaphore_wait(barrier, 3 + jnp.where(first, others, 0))

    for offset in OFFSETS:

        @pl.when(jnp.logical_not(has_sector(-offset)))
        def _():
            inbox[pl.ds(2 * offset + 4, 2)] = jnp.zeros((2, *inbox.shape[1:]), F32)
            inmid[pl.ds(2 * offset + 4, 2)] = jnp.zeros((2, *inmid.shape[1:]), F32)
            inlast[pl.ds(2 * offset + 4, 2)] = jnp.zeros((2, *inlast.shape[1:]), F32)

    def state_hop(way, dist, part_rows, index):
        sign = 1 if way == 0 else -1
        owner = lax.rem(pan - sign * 2 * (dist - 1) + panels, panels)
        return pltpu.make_async_remote_copy(
            src_ref=mbuf.at[owner, part_rows],
            dst_ref=mbuf.at[owner, part_rows],
            send_sem=s_send.at[way],
            recv_sem=s_recv.at[way, index],
            device_id=(sec, ahead if way == 0 else behind),
            device_id_type=MESH,
        )

    def state_arrival(way, dist, part_rows, index):
        sign = 1 if way == 0 else -1
        owner = lax.rem(pan - sign * 2 * dist + 2 * panels, panels)
        return pltpu.make_async_remote_copy(
            src_ref=mbuf.at[owner, part_rows],
            dst_ref=mbuf.at[owner, part_rows],
            send_sem=s_send.at[way],
            recv_sem=s_recv.at[way, index],
            device_id=(sec, ahead if way == 0 else behind),
            device_id_type=MESH,
        )

    def state_rows(way, dist):
        if dist < 4:
            return pl.ds(0, rows)
        return pl.ds(way * half, half)

    def slot(way, dist):
        if dist == 0:
            return 0
        return ring_size - dist if way == 0 else dist

    def goes(way, piece, target):
        target = lax.rem(target + ring_size, ring_size)
        ahead_pieces = jnp.where(target < EARLY, EARLY_PIECES, PIECES // 2)
        return piece < ahead_pieces if way == 0 else piece >= ahead_pieces

    def ring_hop(way, dist, chunk):
        if dist < 4:
            piece = pl.ds(chunk * per_chunk, per_chunk)
        else:
            piece = pl.ds(last_from[chunk], LAST_TERMS[chunk])
        return pltpu.make_async_remote_copy(
            src_ref=ring.at[slot(way, dist - 1), piece],
            dst_ref=ring.at[slot(way, dist), piece],
            send_sem=r_send.at[way] if dist < 4 else l_send.at[way, chunk],
            recv_sem=r_recv.at[way, (dist - 1) * CHUNKS + chunk] if dist < 4 else l_recv.at[chunk],
            device_id=(sec, ahead if way == 0 else behind),
            device_id_type=MESH,
        )

    def send_state(dist):
        for way in range(2):
            state_hop(way, dist, state_rows(way, dist), dist - 1).start()

    def wait_state(dist):
        for way in range(2):
            state_arrival(way, dist, state_rows(way, dist), dist - 1).wait_recv()

    def hop(dist):
        for way in (1, 0):
            state_arrival(way, dist, state_rows(way, dist), dist - 1).wait_recv()
            state_hop(way, dist + 1, state_rows(way, dist + 1), dist).start()
            ring_hop(way, 1, dist).start()

    def send_own(chunk):
        for way in range(2):
            ring_hop(way, 1, chunk).start()

    def service(dist, chunk):
        for way in (1, 0):
            ring_hop(way, dist, chunk).wait_recv()
            if dist < 3:
                ring_hop(way, dist + 1, chunk).start()
            else:
                for piece in range(PIECES):
                    if (last_from[piece] + LAST_TERMS[piece] - 1) // per_chunk == chunk:

                        @pl.when(goes(way, piece, zed + 1 if way == 0 else zed - 1))
                        def _():
                            ring_hop(way, 4, piece).start()

    with jax.named_scope("own_state"):
        copy_state.wait()
        send_state(1)
    with jax.named_scope("own_right"):
        copy_right.wait()
        send_own(0)


    for copy in tables:
        copy.wait()
    live = sdims[0, 0]
    lanes = channels * half
    slot_row = (vout[...] - sec + 2).astype(F32)
    table = jnp.concatenate(
        [slot_row, vterm[...].astype(F32), vcoup[...].astype(F32), jnp.zeros((5, channels), F32)], axis=0
    ).astype(BF16)
    chan_of_lane = lax.broadcasted_iota(jnp.int32, (channels, lanes), 1) // half
    chan = lax.broadcasted_iota(jnp.int32, (channels, lanes), 0)
    spread = jnp.where(chan_of_lane == chan, 1.0, 0.0).astype(BF16)
    wide = jnp.dot(table, spread, preferred_element_type=F32)
    row_in_half = lax.rem(lax.broadcasted_iota(jnp.int32, (1, lanes), 1), half).astype(F32)
    target = (wide[1:2] * 5.0 + wide[0:1]) * float(half) + row_in_half
    weight = wide[2:3]

    tile = 256

    def combine(step):
        at = lax.broadcasted_iota(jnp.int32, (tile, lanes), 0).astype(F32) + float(step * tile)
        kron = jnp.where(at == target, weight, 0.0).astype(BF16)
        for g in range(2):
            made = jnp.dot(kron, lbuf[g].reshape(lanes, width), preferred_element_type=F32).astype(BF16)
            groups = tile // half
            cbuf[pl.ds(step * groups, groups), g] = made.reshape(groups, half, width)

    pltpu.make_async_copy(lbuf, lbuf, local_sem.at[2]).wait()
    with jax.named_scope("combine_a"):
        combine(0)
        combine(1)
    with jax.named_scope("hop_1"):
        hop(1)
    combine(2)
    combine(3)
    with jax.named_scope("hop_2"):
        hop(2)
    combine(4)
    with jax.named_scope("hop_3"):
        hop(3)
    service(1, 0)
    with jax.named_scope("hop_4"):
        wait_state(4)

    def pair_copy(step):
        return pltpu.make_async_remote_copy(
            src_ref=mbuf.at[2 * step + core],
            dst_ref=mbuf.at[2 * step + core],
            send_sem=pair_send,
            recv_sem=pair_recv,
            device_id=(sec, partner),
            device_id_type=MESH,
        )

    for step in range(ring_size):
        pair_copy(step).start()
    for offset in OFFSETS:

        @pl.when(first & has_sector(offset))
        def _():
            for other in (pan, partner):
                pl.semaphore_signal(
                    column_sem, inc=1, device_id=(sector_at(offset), other), device_id_type=MESH
                )

    service(1, 1)
    pair_all = pltpu.make_async_remote_copy(
        src_ref=mbuf.at[pl.ds(0, ring_size)],
        dst_ref=mbuf.at[pl.ds(0, ring_size)],
        send_sem=pair_send,
        recv_sem=pair_recv,
        device_id=(sec, partner),
        device_id_type=MESH,
    )
    pair_all.wait_recv()

    row_at = lax.broadcasted_iota(jnp.int32, (width, width), 0)
    col_at = lax.broadcasted_iota(jnp.int32, (width, width), 1)
    masked = jnp.where(
        (row_at < live) & (col_at < live), mbuf[...].reshape(width, width), jnp.zeros((), BF16)
    )
    mfull[...] = masked
    group = 4
    for step in range(terms // group):
        block = cbuf[pl.ds(step * group * 5, group * 5)].reshape(group * 5 * rows, width)
        made = jnp.dot(block, mfull[...], preferred_element_type=F32).astype(BF16)
        xbuf[pl.ds(step * group, group), core] = made.reshape(group, 5 * rows, width)
        if step % 2:
            service(1, 2 + step // 2)
        pltpu.make_async_remote_copy(
            src_ref=xbuf.at[pl.ds(step * group, group), core],
            dst_ref=xbuf.at[pl.ds(step * group, group), core],
            send_sem=x_send,
            recv_sem=x_recv,
            device_id=(sec, partner),
            device_id_type=MESH,
        ).start()
    x_all = pltpu.make_async_remote_copy(
        src_ref=xbuf.at[:, core],
        dst_ref=xbuf.at[:, core],
        send_sem=x_send,
        recv_sem=x_recv,
        device_id=(sec, partner),
        device_id_type=MESH,
    )

    @pl.when(first)
    def _():
        pl.semaphore_wait(column_sem, others)
        for step in range(1, ring_size):
            pl.semaphore_signal(
                ready_sem, inc=1, device_id=(sec, 2 * step + core), device_id_type=MESH
            )

    part[...] = jnp.zeros(part.shape, F32)
    x_all.wait_recv()

    def contract(slots, which, held):
        blocks = []
        for w in which:
            pieces = [ring[k, w] for k in slots]
            blocks.append(pieces[0] if len(pieces) == 1 else jnp.concatenate(pieces, axis=0))
        totals = []
        for owner in range(2):
            total = None if held is None else held[owner]
            for w, block in zip(which, blocks):
                product = nt_dot(xbuf[w, owner], block)
                total = product if total is None else total + product
            totals.append(total)
        return totals

    def place(slots, totals):
        for owner, total in enumerate(totals):
            for i, k in enumerate(slots):
                piece = total[:, i * cols : (i + 1) * cols].reshape(5, rows, cols)
                part[pl.ds(owner * 5, 5), :, pl.ds(k * cols, cols)] = piece

    def keep_in(acc, totals):
        for owner, total in enumerate(totals):
            acc[owner] = total

    def pack(total):
        total = total.reshape(5, rows // 8, 8, cols)
        return jnp.concatenate([total[:, i] for i in range(rows // 8)], axis=2)

    def unpack(packed):
        return jnp.concatenate([packed[:, i * cols : (i + 1) * cols] for i in range(rows // 8)], axis=0)

    def exchange(source, landing, send_sem, recv_sem):
        def copy_to(which, j):
            return pltpu.make_async_remote_copy(
                src_ref=source.at[which * 5 + j],
                dst_ref=landing.at[2 * j + core],
                send_sem=send_sem,
                recv_sem=recv_sem,
                device_id=(sector_at(j - 2), 2 * zed + which),
                device_id_type=MESH,
            )

        def start():
            for j in (0, 4, 1, 3):

                @pl.when(has_sector(j - 2))
                def _():
                    for which in range(2):
                        copy_to(which, j).start()

            copy_to(1 - core, 2).start()

        def wait_all(wait):
            for count in (4, 6, 8):

                @pl.when(others == count)
                def _():
                    wait(
                        pltpu.make_async_remote_copy(
                            src_ref=source.at[pl.ds(0, count + 1)],
                            dst_ref=landing.at[pl.ds(0, count + 1)],
                            send_sem=send_sem,
                            recv_sem=recv_sem,
                            device_id=(sec, partner),
                            device_id_type=MESH,
                        )
                    )

        def wait_recv():
            wait_all(lambda copy: copy.wait_recv())

        def wait_send():
            wait_all(lambda copy: copy.wait_send())

        return start, wait_recv, wait_send

    def sum_of(landing, cls):
        total = landing[cls]
        for j in range(1, 5):
            total = total + landing[2 * j + cls]
        return total

    start_a, recv_a, sent_a = exchange(part, inbox, a_send, a_recv)
    start_m, recv_m, sent_m = exchange(mid, inmid, m_send, m_recv)
    start_b, recv_b, sent_b = exchange(last, inlast, b_send, b_recv)

    def chunk_terms(chunk):
        return range(chunk * per_chunk, (chunk + 1) * per_chunk)

    with jax.named_scope("contract_a"):
        place((0, 1, 7), contract((0, 1, 7), range(terms), None))
    with jax.named_scope("ring_2"):
        for chunk in range(CHUNKS):
            service(2, chunk)
            totals = contract((2, 6), chunk_terms(chunk), acc2 if chunk else None)
            if chunk < CHUNKS - 1:
                keep_in(acc2, totals)
            else:
                place((2, 6), totals)
    with jax.named_scope("ring_3"):
        for chunk in range(CHUNKS):
            service(3, chunk)
            if chunk == 0:

                @pl.when(jnp.logical_not(first))
                def _():
                    pl.semaphore_wait(ready_sem, 1)

                start_a()
            keep_in(acc3, contract((3, 5), chunk_terms(chunk), acc3 if chunk else None))
        for owner in range(2):
            for i in range(2):
                mid[pl.ds(owner * 5, 5), pl.ds(8 * i, 8)] = pack(acc3[owner, :, pl.ds(i * cols, cols)])

    def by_final_step(step):
        return [
            w
            for piece in (step, PIECES // 2 + step)
            for w in range(last_from[piece], last_from[piece] + LAST_TERMS[piece])
        ]

    def final_wait(step):
        for piece in (step, PIECES // 2 + step):
            ring_hop(0, 4, piece).wait_recv()

    final_wait(0)
    start_m()
    keep_in(acc4, contract((4,), by_final_step(0), None))
    for step in range(1, PIECES // 2 - 1):
        final_wait(step)
        keep_in(acc4, contract((4,), by_final_step(step), acc4))
    with jax.named_scope("final_wait"):
        final_wait(PIECES // 2 - 1)
    with jax.named_scope("last"):
        totals = contract((4,), by_final_step(PIECES // 2 - 1), acc4)
        for owner in range(2):
            last[pl.ds(owner * 5, 5)] = pack(totals[owner])
        start_b()

    recv_a()
    inbox[4 + core] = part[core * 5 + 2]
    inmid[4 + core] = mid[core * 5 + 2]
    inlast[4 + core] = last[core * 5 + 2]
    recv_m()
    sums = []
    for cls in range(2):
        total = sum_of(inbox, cls)
        extra = sum_of(inmid, cls)
        total = jnp.concatenate(
            [
                total[:, : 3 * cols],
                unpack(extra[:8]),
                total[:, 4 * cols : 5 * cols],
                unpack(extra[8:]),
                total[:, 6 * cols :],
            ],
            axis=1,
        )
        sums.append(pltpu.roll(total, zed * cols, axis=1))
    pieces = []
    for k in range(ring_size):
        for cls in range(2):
            pieces.append(sums[cls][:, k * cols : (k + 1) * cols])
    early = jnp.concatenate(pieces, axis=1)
    lane = lax.broadcasted_iota(jnp.int32, (rows, width), 1)
    here = lane // (2 * cols) == lax.rem(zed + 4, ring_size)
    with jax.named_scope("sent"):
        for way in range(2):
            pltpu.make_async_remote_copy(
                src_ref=mbuf.at[pl.ds(0, 7), pl.ds(0, half)],
                dst_ref=mbuf.at[pl.ds(0, 7), pl.ds(0, half)],
                send_sem=s_send.at[way],
                recv_sem=s_recv.at[way, 0],
                device_id=(sec, partner),
                device_id_type=MESH,
            ).wait_send()
            pltpu.make_async_remote_copy(
                src_ref=ring.at[pl.ds(0, 3)],
                dst_ref=ring.at[pl.ds(0, 3)],
                send_sem=r_send.at[way],
                recv_sem=r_recv.at[way, 0],
                device_id=(sec, partner),
                device_id_type=MESH,
            ).wait_send()
            for piece in range(PIECES):

                @pl.when(goes(way, piece, zed + 1 if way == 0 else zed - 1))
                def _():
                    ring_hop(way, 4, piece).wait_send()

        pair_all.wait_send()
        x_all.wait_send()
        sent_a()
        sent_m()
        sent_b()
    with jax.named_scope("recv_b"):
        recv_b()
    with jax.named_scope("finish"):
        lasts = [unpack(sum_of(inlast, cls)) for cls in range(2)]
        late = jnp.concatenate(lasts * (width // (2 * cols)), axis=1)
        out_ref[0] = early + jnp.where(here, late, 0.0)


def on_device(
    wave_state, right_blocks, left_blocks, coupling, channel_term, channel_out, sector_dims
):
    _, rows, width = wave_state.shape
    _, terms, _, cols = right_blocks.shape
    channels = left_blocks.shape[0]
    panels = lax.axis_size("pan")
    ring_size = panels // 2
    half = rows // 2
    right = jnp.swapaxes(right_blocks[0], 1, 2)
    dma = pltpu.SemaphoreType.DMA
    applied = pl.pallas_call(
        kernel,
        out_shape=pltpu.VMEM((1, rows, width), F32),
        in_specs=[pl.BlockSpec(memory_space=pltpu.HBM)] * 7,
        out_specs=pl.BlockSpec(memory_space=pltpu.VMEM),
        scratch_shapes=[
            pltpu.VMEM((ring_size, terms, cols, width), BF16),
            pltpu.VMEM((panels, rows, width), BF16),
            pltpu.VMEM((width, width), BF16),
            pltpu.VMEM((2, channels, half, width), BF16),
            pltpu.VMEM((5 * terms, 2, half, width), BF16),
            pltpu.VMEM((terms, 2, 5 * rows, width), BF16),
            pltpu.VMEM((10, rows, ring_size * cols), F32),
            pltpu.VMEM((2, 5 * rows, 2 * cols), F32),
            pltpu.VMEM((2, 5 * rows, 2 * cols), F32),
            pltpu.VMEM((2, 5 * rows, cols), F32),
            pltpu.VMEM((10, rows, ring_size * cols), F32),
            pltpu.VMEM((10, 16, rows // 8 * cols), F32),
            pltpu.VMEM((10, 16, rows // 8 * cols), F32),
            pltpu.VMEM((10, 8, rows // 8 * cols), F32),
            pltpu.VMEM((10, 8, rows // 8 * cols), F32),
            pltpu.VMEM((1, channels), BF16),
            pltpu.VMEM((1, channels), jnp.int32),
            pltpu.VMEM((1, channels), jnp.int32),
            pltpu.SMEM((1, 1), jnp.int32),
            dma((7,)),
            dma((2,)),
            dma((2, 4)),
            dma((2,)),
            dma((2, 3 * CHUNKS)),
            dma((2, PIECES)),
            dma((PIECES,)),
            dma(()),
            dma(()),
            dma(()),
            dma(()),
            dma(()),
            dma(()),
            dma(()),
            dma(()),
            dma(()),
            dma(()),
            pltpu.SemaphoreType.REGULAR,
            pltpu.SemaphoreType.REGULAR,
        ],
        compiler_params=pltpu.CompilerParams(
            collective_id=0, has_side_effects=True, vmem_limit_bytes=60 * 1024 * 1024
        ),
        name="sector_step",
    )(
        wave_state,
        right,
        left_blocks,
        coupling[None],
        channel_term[None],
        channel_out[None],
        sector_dims[None],
    )
    live = sector_dims[0]
    row_ids = lax.axis_index("pan") * rows + lax.iota(jnp.int32, rows)
    kept_mask = (row_ids[:, None] < live) & (lax.iota(jnp.int32, width)[None, :] < live)
    return jnp.where(kept_mask[None], applied, jnp.zeros((), F32))


def solution(mesh):
    return jax.shard_map(
        on_device,
        mesh=mesh,
        in_specs=(
            P("sec", "pan", None),
            P("sec", None, None, "pan"),
            P("sec", "pan", None),
            P("sec"),
            P("sec"),
            P("sec"),
            P("sec"),
        ),
        out_specs=P("sec", "pan", None),
        check_vma=False,
    )
```

```python
import jax
import jax.numpy as jnp
from jax import lax
from jax.experimental import pallas as pl
from jax.experimental.pallas import tpu as pltpu
from jax.sharding import PartitionSpec as P

MESH = pl.DeviceIdType.MESH
F32 = jnp.float32
BF16 = jnp.bfloat16
OFFSETS = (-2, -1, 1, 2)
CHUNKS = 4
LAST_TERMS = (3, 2, 2, 1, 3, 2, 2, 1)
PIECES = len(LAST_TERMS)
EARLY_PIECES = (2, 3)


def nt_dot(lhs, rhs):
    return lax.dot_general(lhs, rhs, (((1,), (1,)), ((), ())), preferred_element_type=F32)


def kernel(
    state, right, left, coup, term, outc, dims,
    out_ref,
    ring, mbuf, mfull, lbuf, cbuf, xbuf, part, acc2, acc3, acc4, inbox, mid, inmid, last, inlast,
    vcoup, vterm, vout, sdims,
    local_sem, s_send, s_recv, r_send, r_recv, l_send, l_recv, pair_send, pair_recv,
    x_send, x_recv, a_send, a_recv, m_send, m_recv, b_send, b_recv, column_sem, ready_sem,
):
    sectors = lax.axis_size("sec")
    panels = lax.axis_size("pan")
    ring_size = panels // 2
    terms, cols, width = right.shape
    channels, rows, _ = left.shape
    sec = lax.axis_index("sec")
    pan = lax.axis_index("pan")
    zed = pan // 2
    core = lax.rem(pan, 2)
    partner = pan + 1 - 2 * core
    ahead = lax.rem(pan + 2, panels)
    behind = lax.rem(pan + panels - 2, panels)
    half = rows // 2
    per_chunk = terms // CHUNKS
    last_from = [sum(LAST_TERMS[:i]) for i in range(PIECES)]

    def sector_at(offset):
        return lax.rem(sec + offset + sectors, sectors)

    def has_sector(offset):
        return (sec + offset >= 0) & (sec + offset < sectors)

    copy_right = pltpu.make_async_copy(right, ring.at[0], local_sem.at[0])
    copy_state = pltpu.make_async_copy(state.at[0], mbuf.at[pan], local_sem.at[1])
    copy_left = [
        pltpu.make_async_copy(left.at[:, pl.ds(g * half, half), :], lbuf.at[g], local_sem.at[2])
        for g in range(2)
    ]
    tables = [
        pltpu.make_async_copy(coup, vcoup, local_sem.at[3]),
        pltpu.make_async_copy(term, vterm, local_sem.at[4]),
        pltpu.make_async_copy(outc, vout, local_sem.at[5]),
        pltpu.make_async_copy(dims, sdims, local_sem.at[6]),
    ]
    barrier = pltpu.get_barrier_semaphore()
    first = zed == 0
    for peer in (ahead, behind, partner):
        pl.semaphore_signal(barrier, inc=1, device_id=(sec, peer), device_id_type=MESH)
    others = 0
    for offset in OFFSETS:
        exists = has_sector(offset)
        others = others + 2 * jnp.where(exists, 1, 0)

        @pl.when(first & exists)
        def _():
            for other in (pan, partner):
                pl.semaphore_signal(
                    barrier, inc=1, device_id=(sector_at(offset), other), device_id_type=MESH
                )

    copy_state.start()
    copy_right.start()
    for copy in tables:
        copy.start()
    for copy in copy_left:
        copy.start()

    with jax.named_scope("barrier"):
        pl.semaphore_wait(barrier, 3 + jnp.where(first, others, 0))

    for offset in OFFSETS:

        @pl.when(jnp.logical_not(has_sector(-offset)))
        def _():
            inbox[pl.ds(2 * offset + 4, 2)] = jnp.zeros((2, *inbox.shape[1:]), F32)
            inmid[pl.ds(2 * offset + 4, 2)] = jnp.zeros((2, *inmid.shape[1:]), F32)
            inlast[pl.ds(2 * offset + 4, 2)] = jnp.zeros((2, *inlast.shape[1:]), F32)

    def state_hop(way, dist, part_rows, index):
        sign = 1 if way == 0 else -1
        owner = lax.rem(pan - sign * 2 * (dist - 1) + panels, panels)
        return pltpu.make_async_remote_copy(
            src_ref=mbuf.at[owner, part_rows],
            dst_ref=mbuf.at[owner, part_rows],
            send_sem=s_send.at[way],
            recv_sem=s_recv.at[way, index],
            device_id=(sec, ahead if way == 0 else behind),
            device_id_type=MESH,
        )

    def state_arrival(way, dist, part_rows, index):
        sign = 1 if way == 0 else -1
        owner = lax.rem(pan - sign * 2 * dist + 2 * panels, panels)
        return pltpu.make_async_remote_copy(
            src_ref=mbuf.at[owner, part_rows],
            dst_ref=mbuf.at[owner, part_rows],
            send_sem=s_send.at[way],
            recv_sem=s_recv.at[way, index],
            device_id=(sec, ahead if way == 0 else behind),
            device_id_type=MESH,
        )

    def state_rows(way, dist):
        if dist < 4:
            return pl.ds(0, rows)
        return pl.ds(way * half, half)

    def slot(way, dist):
        if dist == 0:
            return 0
        return ring_size - dist if way == 0 else dist

    def goes(way, piece, target):
        target = lax.rem(target + ring_size, ring_size)
        ahead_pieces = PIECES // 2
        for place, pieces in enumerate(EARLY_PIECES):
            ahead_pieces = jnp.where(target == place, pieces, ahead_pieces)
        return piece < ahead_pieces if way == 0 else piece >= ahead_pieces

    def ring_hop(way, dist, chunk):
        if dist < 4:
            piece = pl.ds(chunk * per_chunk, per_chunk)
        else:
            piece = pl.ds(last_from[chunk], LAST_TERMS[chunk])
        return pltpu.make_async_remote_copy(
            src_ref=ring.at[slot(way, dist - 1), piece],
            dst_ref=ring.at[slot(way, dist), piece],
            send_sem=r_send.at[way] if dist < 4 else l_send.at[way],
            recv_sem=r_recv.at[way, (dist - 1) * CHUNKS + chunk] if dist < 4 else l_recv.at[chunk],
            device_id=(sec, ahead if way == 0 else behind),
            device_id_type=MESH,
        )

    def send_state(dist):
        for way in range(2):
            state_hop(way, dist, state_rows(way, dist), dist - 1).start()

    def wait_state(dist):
        for way in range(2):
            state_arrival(way, dist, state_rows(way, dist), dist - 1).wait_recv()

    def hop(dist, way):
        state_arrival(way, dist, state_rows(way, dist), dist - 1).wait_recv()
        state_hop(way, dist + 1, state_rows(way, dist + 1), dist).start()
        if way == 0:
            ring_hop(way, 1, dist).start()
        else:

            @pl.when(jnp.logical_not(leads))
            def _():
                ring_hop(way, 1, dist).start()

            if dist + 1 < CHUNKS:

                @pl.when(leads)
                def _():
                    ring_hop(way, 1, dist + 1).start()

    leads = (zed == 1) | (zed == 2)

    def send_own(chunk):
        for way in range(2):
            ring_hop(way, 1, chunk).start()

    def service(dist, chunk, ways=(1, 0)):
        for way in ways:
            ring_hop(way, dist, chunk).wait_recv()
            if dist < 3:
                ring_hop(way, dist + 1, chunk).start()
            else:
                for piece in range(PIECES):
                    if (last_from[piece] + LAST_TERMS[piece] - 1) // per_chunk == chunk:

                        @pl.when(goes(way, piece, zed + 1 if way == 0 else zed - 1))
                        def _():
                            ring_hop(way, 4, piece).start()

    with jax.named_scope("own_state"):
        copy_state.wait()
        send_state(1)
    with jax.named_scope("own_right"):
        copy_right.wait()
        send_own(0)

        @pl.when(leads)
        def _():
            ring_hop(1, 1, 1).start()


    for copy in tables:
        copy.wait()
    live = sdims[0, 0]
    lanes = channels * half
    slot_row = (vout[...] - sec + 2).astype(F32)
    table = jnp.concatenate(
        [slot_row, vterm[...].astype(F32), vcoup[...].astype(F32), jnp.zeros((5, channels), F32)], axis=0
    ).astype(BF16)
    chan_of_lane = lax.broadcasted_iota(jnp.int32, (channels, lanes), 1) // half
    chan = lax.broadcasted_iota(jnp.int32, (channels, lanes), 0)
    spread = jnp.where(chan_of_lane == chan, 1.0, 0.0).astype(BF16)
    wide = jnp.dot(table, spread, preferred_element_type=F32)
    row_in_half = lax.rem(lax.broadcasted_iota(jnp.int32, (1, lanes), 1), half).astype(F32)
    target = (wide[1:2] * 5.0 + wide[0:1]) * float(half) + row_in_half
    weight = wide[2:3]

    tile = 256

    def combine(step):
        at = lax.broadcasted_iota(jnp.int32, (tile, lanes), 0).astype(F32) + float(step * tile)
        kron = jnp.where(at == target, weight, 0.0).astype(BF16)
        for g in range(2):
            made = jnp.dot(kron, lbuf[g].reshape(lanes, width), preferred_element_type=F32).astype(BF16)
            groups = tile // half
            cbuf[pl.ds(step * groups, groups), g] = made.reshape(groups, half, width)

    pltpu.make_async_copy(lbuf, lbuf, local_sem.at[2]).wait()
    with jax.named_scope("combine_a"):
        combine(0)
        combine(1)
    with jax.named_scope("hop_1"):
        hop(1, 1)
        hop(1, 0)
    combine(2)
    combine(3)
    with jax.named_scope("hop_2"):
        hop(2, 1)
        hop(2, 0)
    combine(4)
    with jax.named_scope("hop_3"):
        hop(3, 1)
        service(1, 0, (1,))
        service(1, 1, (1,))
        hop(3, 0)
    service(1, 0, (0,))
    service(1, 1, (0,))
    with jax.named_scope("hop_4"):
        wait_state(4)

    def pair_copy(step):
        return pltpu.make_async_remote_copy(
            src_ref=mbuf.at[2 * step + core],
            dst_ref=mbuf.at[2 * step + core],
            send_sem=pair_send,
            recv_sem=pair_recv,
            device_id=(sec, partner),
            device_id_type=MESH,
        )

    for step in range(ring_size):
        pair_copy(step).start()
    for offset in OFFSETS:

        @pl.when(first & has_sector(offset))
        def _():
            for other in (pan, partner):
                pl.semaphore_signal(
                    column_sem, inc=1, device_id=(sector_at(offset), other), device_id_type=MESH
                )

    pair_all = pltpu.make_async_remote_copy(
        src_ref=mbuf.at[pl.ds(0, ring_size)],
        dst_ref=mbuf.at[pl.ds(0, ring_size)],
        send_sem=pair_send,
        recv_sem=pair_recv,
        device_id=(sec, partner),
        device_id_type=MESH,
    )
    pair_all.wait_recv()

    row_at = lax.broadcasted_iota(jnp.int32, (width, width), 0)
    col_at = lax.broadcasted_iota(jnp.int32, (width, width), 1)
    masked = jnp.where(
        (row_at < live) & (col_at < live), mbuf[...].reshape(width, width), jnp.zeros((), BF16)
    )
    mfull[...] = masked
    group = 4
    for step in range(terms // group):
        block = cbuf[pl.ds(step * group * 5, group * 5)].reshape(group * 5 * rows, width)
        made = jnp.dot(block, mfull[...], preferred_element_type=F32).astype(BF16)
        xbuf[pl.ds(step * group, group), core] = made.reshape(group, 5 * rows, width)
        if step % 2:
            service(1, 2 + step // 2)
        pltpu.make_async_remote_copy(
            src_ref=xbuf.at[pl.ds(step * group, group), core],
            dst_ref=xbuf.at[pl.ds(step * group, group), core],
            send_sem=x_send,
            recv_sem=x_recv,
            device_id=(sec, partner),
            device_id_type=MESH,
        ).start()
    x_all = pltpu.make_async_remote_copy(
        src_ref=xbuf.at[:, core],
        dst_ref=xbuf.at[:, core],
        send_sem=x_send,
        recv_sem=x_recv,
        device_id=(sec, partner),
        device_id_type=MESH,
    )

    @pl.when(first)
    def _():
        pl.semaphore_wait(column_sem, others)
        for step in range(1, ring_size):
            pl.semaphore_signal(
                ready_sem, inc=1, device_id=(sec, 2 * step + core), device_id_type=MESH
            )

    part[...] = jnp.zeros(part.shape, F32)
    x_all.wait_recv()

    def contract(slots, which, held):
        blocks = []
        for w in which:
            pieces = [ring[k, w] for k in slots]
            blocks.append(pieces[0] if len(pieces) == 1 else jnp.concatenate(pieces, axis=0))
        totals = []
        for owner in range(2):
            total = None if held is None else held[owner]
            for w, block in zip(which, blocks):
                product = nt_dot(xbuf[w, owner], block)
                total = product if total is None else total + product
            totals.append(total)
        return totals

    def place(slots, totals):
        for owner, total in enumerate(totals):
            for i, k in enumerate(slots):
                piece = total[:, i * cols : (i + 1) * cols].reshape(5, rows, cols)
                part[pl.ds(owner * 5, 5), :, pl.ds(k * cols, cols)] = piece

    def keep_in(acc, totals):
        for owner, total in enumerate(totals):
            acc[owner] = total

    def pack(total):
        total = total.reshape(5, rows // 8, 8, cols)
        return jnp.concatenate([total[:, i] for i in range(rows // 8)], axis=2)

    def unpack(packed):
        return jnp.concatenate([packed[:, i * cols : (i + 1) * cols] for i in range(rows // 8)], axis=0)

    def exchange(source, landing, send_sem, recv_sem):
        def copy_to(which, j):
            return pltpu.make_async_remote_copy(
                src_ref=source.at[which * 5 + j],
                dst_ref=landing.at[2 * j + core],
                send_sem=send_sem,
                recv_sem=recv_sem,
                device_id=(sector_at(j - 2), 2 * zed + which),
                device_id_type=MESH,
            )

        def start():
            for j in (0, 4, 1, 3):

                @pl.when(has_sector(j - 2))
                def _():
                    for which in range(2):
                        copy_to(which, j).start()

            copy_to(1 - core, 2).start()

        def wait_all(wait):
            for count in (4, 6, 8):

                @pl.when(others == count)
                def _():
                    wait(
                        pltpu.make_async_remote_copy(
                            src_ref=source.at[pl.ds(0, count + 1)],
                            dst_ref=landing.at[pl.ds(0, count + 1)],
                            send_sem=send_sem,
                            recv_sem=recv_sem,
                            device_id=(sec, partner),
                            device_id_type=MESH,
                        )
                    )

        def wait_recv():
            wait_all(lambda copy: copy.wait_recv())

        def wait_send():
            wait_all(lambda copy: copy.wait_send())

        return start, wait_recv, wait_send

    def sum_of(landing, cls):
        total = landing[cls]
        for j in range(1, 5):
            total = total + landing[2 * j + cls]
        return total

    start_a, recv_a, sent_a = exchange(part, inbox, a_send, a_recv)
    start_m, recv_m, sent_m = exchange(mid, inmid, m_send, m_recv)
    start_b, recv_b, sent_b = exchange(last, inlast, b_send, b_recv)

    def chunk_terms(chunk):
        return range(chunk * per_chunk, (chunk + 1) * per_chunk)

    with jax.named_scope("contract_a"):
        place((0, 1, 7), contract((0, 1, 7), range(terms), None))
    with jax.named_scope("ring_2"):
        for chunk in range(CHUNKS):
            service(2, chunk)
            totals = contract((2, 6), chunk_terms(chunk), acc2 if chunk else None)
            if chunk < CHUNKS - 1:
                keep_in(acc2, totals)
            else:
                place((2, 6), totals)
    with jax.named_scope("ring_3"):
        for chunk in range(CHUNKS):
            service(3, chunk)
            if chunk == 0:

                @pl.when(jnp.logical_not(first))
                def _():
                    pl.semaphore_wait(ready_sem, 1)

                start_a()
            keep_in(acc3, contract((3, 5), chunk_terms(chunk), acc3 if chunk else None))
        for owner in range(2):
            for i in range(2):
                mid[pl.ds(owner * 5, 5), pl.ds(8 * i, 8)] = pack(acc3[owner, :, pl.ds(i * cols, cols)])

    def by_final_step(step):
        return [
            w
            for piece in (step, PIECES // 2 + step)
            for w in range(last_from[piece], last_from[piece] + LAST_TERMS[piece])
        ]

    def final_wait(step):
        for piece in (step, PIECES // 2 + step):
            ring_hop(0, 4, piece).wait_recv()

    final_wait(0)
    start_m()
    keep_in(acc4, contract((4,), by_final_step(0), None))
    for step in range(1, PIECES // 2 - 1):
        final_wait(step)
        keep_in(acc4, contract((4,), by_final_step(step), acc4))
    with jax.named_scope("final_wait"):
        final_wait(PIECES // 2 - 1)
    with jax.named_scope("last"):
        totals = contract((4,), by_final_step(PIECES // 2 - 1), acc4)
        for owner in range(2):
            last[pl.ds(owner * 5, 5)] = pack(totals[owner])
        start_b()

    recv_a()
    inbox[4 + core] = part[core * 5 + 2]
    inmid[4 + core] = mid[core * 5 + 2]
    inlast[4 + core] = last[core * 5 + 2]
    recv_m()
    sums = []
    for cls in range(2):
        total = sum_of(inbox, cls)
        extra = sum_of(inmid, cls)
        total = jnp.concatenate(
            [
                total[:, : 3 * cols],
                unpack(extra[:8]),
                total[:, 4 * cols : 5 * cols],
                unpack(extra[8:]),
                total[:, 6 * cols :],
            ],
            axis=1,
        )
        sums.append(pltpu.roll(total, zed * cols, axis=1))
    pieces = []
    for k in range(ring_size):
        for cls in range(2):
            pieces.append(sums[cls][:, k * cols : (k + 1) * cols])
    early = jnp.concatenate(pieces, axis=1)
    lane = lax.broadcasted_iota(jnp.int32, (rows, width), 1)
    here = lane // (2 * cols) == lax.rem(zed + 4, ring_size)
    with jax.named_scope("sent"):
        for way in range(2):
            pltpu.make_async_remote_copy(
                src_ref=mbuf.at[pl.ds(0, 7), pl.ds(0, half)],
                dst_ref=mbuf.at[pl.ds(0, 7), pl.ds(0, half)],
                send_sem=s_send.at[way],
                recv_sem=s_recv.at[way, 0],
                device_id=(sec, partner),
                device_id_type=MESH,
            ).wait_send()
            pltpu.make_async_remote_copy(
                src_ref=ring.at[pl.ds(0, 3)],
                dst_ref=ring.at[pl.ds(0, 3)],
                send_sem=r_send.at[way],
                recv_sem=r_recv.at[way, 0],
                device_id=(sec, partner),
                device_id_type=MESH,
            ).wait_send()
            reached = lax.rem(zed + (1 if way == 0 else ring_size - 1), ring_size)
            for place, ahead_pieces in enumerate((*EARLY_PIECES, PIECES // 2)):
                is_target = reached == place if place < len(EARLY_PIECES) else reached >= place
                count = sum(LAST_TERMS[:ahead_pieces] if way == 0 else LAST_TERMS[ahead_pieces:])

                @pl.when(is_target)
                def _():
                    pltpu.make_async_remote_copy(
                        src_ref=ring.at[0, pl.ds(0, count)],
                        dst_ref=ring.at[0, pl.ds(0, count)],
                        send_sem=l_send.at[way],
                        recv_sem=l_recv.at[0],
                        device_id=(sec, partner),
                        device_id_type=MESH,
                    ).wait_send()

        pair_all.wait_send()
        x_all.wait_send()
        sent_a()
        sent_m()
        sent_b()
    with jax.named_scope("recv_b"):
        recv_b()
    with jax.named_scope("finish"):
        lasts = [unpack(sum_of(inlast, cls)) for cls in range(2)]
        late = jnp.concatenate(lasts * (width // (2 * cols)), axis=1)
        out_ref[0] = early + jnp.where(here, late, 0.0)


def on_device(
    wave_state, right_blocks, left_blocks, coupling, channel_term, channel_out, sector_dims
):
    _, rows, width = wave_state.shape
    _, terms, _, cols = right_blocks.shape
    channels = left_blocks.shape[0]
    panels = lax.axis_size("pan")
    ring_size = panels // 2
    half = rows // 2
    right = jnp.swapaxes(right_blocks[0], 1, 2)
    dma = pltpu.SemaphoreType.DMA
    applied = pl.pallas_call(
        kernel,
        out_shape=pltpu.VMEM((1, rows, width), F32),
        in_specs=[pl.BlockSpec(memory_space=pltpu.HBM)] * 7,
        out_specs=pl.BlockSpec(memory_space=pltpu.VMEM),
        scratch_shapes=[
            pltpu.VMEM((ring_size, terms, cols, width), BF16),
            pltpu.VMEM((panels, rows, width), BF16),
            pltpu.VMEM((width, width), BF16),
            pltpu.VMEM((2, channels, half, width), BF16),
            pltpu.VMEM((5 * terms, 2, half, width), BF16),
            pltpu.VMEM((terms, 2, 5 * rows, width), BF16),
            pltpu.VMEM((10, rows, ring_size * cols), F32),
            pltpu.VMEM((2, 5 * rows, 2 * cols), F32),
            pltpu.VMEM((2, 5 * rows, 2 * cols), F32),
            pltpu.VMEM((2, 5 * rows, cols), F32),
            pltpu.VMEM((10, rows, ring_size * cols), F32),
            pltpu.VMEM((10, 16, rows // 8 * cols), F32),
            pltpu.VMEM((10, 16, rows // 8 * cols), F32),
            pltpu.VMEM((10, 8, rows // 8 * cols), F32),
            pltpu.VMEM((10, 8, rows // 8 * cols), F32),
            pltpu.VMEM((1, channels), BF16),
            pltpu.VMEM((1, channels), jnp.int32),
            pltpu.VMEM((1, channels), jnp.int32),
            pltpu.SMEM((1, 1), jnp.int32),
            dma((7,)),
            dma((2,)),
            dma((2, 4)),
            dma((2,)),
            dma((2, 3 * CHUNKS)),
            dma((2,)),
            dma((PIECES,)),
            dma(()),
            dma(()),
            dma(()),
            dma(()),
            dma(()),
            dma(()),
            dma(()),
            dma(()),
            dma(()),
            dma(()),
            pltpu.SemaphoreType.REGULAR,
            pltpu.SemaphoreType.REGULAR,
        ],
        compiler_params=pltpu.CompilerParams(
            collective_id=0, has_side_effects=True, vmem_limit_bytes=60 * 1024 * 1024
        ),
        name="sector_step",
    )(
        wave_state,
        right,
        left_blocks,
        coupling[None],
        channel_term[None],
        channel_out[None],
        sector_dims[None],
    )
    live = sector_dims[0]
    row_ids = lax.axis_index("pan") * rows + lax.iota(jnp.int32, rows)
    kept_mask = (row_ids[:, None] < live) & (lax.iota(jnp.int32, width)[None, :] < live)
    return jnp.where(kept_mask[None], applied, jnp.zeros((), F32))


def solution(mesh):
    return jax.shard_map(
        on_device,
        mesh=mesh,
        in_specs=(
            P("sec", "pan", None),
            P("sec", None, None, "pan"),
            P("sec", "pan", None),
            P("sec"),
            P("sec"),
            P("sec"),
            P("sec"),
        ),
        out_specs=P("sec", "pan", None),
        check_vma=False,
    )
```

```python
import jax
import jax.numpy as jnp
from jax import lax
from jax.experimental import pallas as pl
from jax.experimental.pallas import tpu as pltpu
from jax.sharding import PartitionSpec as P

MESH = pl.DeviceIdType.MESH
F32 = jnp.float32
BF16 = jnp.bfloat16
OFFSETS = (-2, -1, 1, 2)
CHUNKS = 4
LAST_TERMS = (3, 2, 2, 1, 3, 2, 2, 1)
PIECES = len(LAST_TERMS)
EARLY_PIECES = (2, 3)


def nt_dot(lhs, rhs):
    return lax.dot_general(lhs, rhs, (((1,), (1,)), ((), ())), preferred_element_type=F32)


def kernel(
    state, right, left, coup, term, outc, dims,
    out_ref,
    ring, mbuf, mfull, lbuf, cbuf, xbuf, part, acc2, acc3, acc4, inbox, mid, inmid, last, inlast,
    vcoup, vterm, vout, sdims,
    local_sem, s_send, s_recv, r_send, r_recv, l_send, l_recv, pair_send, pair_recv,
    x_send, x_recv, a_send, a_recv, m_send, m_recv, b_send, b_recv, column_sem, ready_sem, later_sem,
):
    sectors = lax.axis_size("sec")
    panels = lax.axis_size("pan")
    ring_size = panels // 2
    terms, cols, width = right.shape
    channels, rows, _ = left.shape
    sec = lax.axis_index("sec")
    pan = lax.axis_index("pan")
    zed = pan // 2
    core = lax.rem(pan, 2)
    partner = pan + 1 - 2 * core
    ahead = lax.rem(pan + 2, panels)
    behind = lax.rem(pan + panels - 2, panels)
    half = rows // 2
    per_chunk = terms // CHUNKS
    last_from = [sum(LAST_TERMS[:i]) for i in range(PIECES)]

    def sector_at(offset):
        return lax.rem(sec + offset + sectors, sectors)

    def has_sector(offset):
        return (sec + offset >= 0) & (sec + offset < sectors)

    copy_right = pltpu.make_async_copy(right, ring.at[0], local_sem.at[0])
    copy_state = pltpu.make_async_copy(state.at[0], mbuf.at[pan], local_sem.at[1])
    copy_left = [
        pltpu.make_async_copy(left.at[:, pl.ds(g * half, half), :], lbuf.at[g], local_sem.at[2])
        for g in range(2)
    ]
    tables = [
        pltpu.make_async_copy(coup, vcoup, local_sem.at[3]),
        pltpu.make_async_copy(term, vterm, local_sem.at[4]),
        pltpu.make_async_copy(outc, vout, local_sem.at[5]),
        pltpu.make_async_copy(dims, sdims, local_sem.at[6]),
    ]
    barrier = pltpu.get_barrier_semaphore()
    first = zed == 0
    pl.semaphore_signal(barrier, inc=1, device_id=(sec, partner), device_id_type=MESH)

    tells_ahead = zed == ring_size - 1
    tells_behind = zed == 2

    @pl.when(jnp.logical_not(tells_ahead))
    def _():
        pl.semaphore_signal(barrier, inc=1, device_id=(sec, ahead), device_id_type=MESH)

    @pl.when(jnp.logical_not(tells_behind))
    def _():
        pl.semaphore_signal(barrier, inc=1, device_id=(sec, behind), device_id_type=MESH)

    others = 0
    for offset in OFFSETS:
        exists = has_sector(offset)
        others = others + 2 * jnp.where(exists, 1, 0)

        @pl.when(first & exists)
        def _():
            for other in (pan, partner):
                pl.semaphore_signal(
                    barrier, inc=1, device_id=(sector_at(offset), other), device_id_type=MESH
                )

    copy_state.start()
    copy_right.start()
    for copy in tables:
        copy.start()
    for copy in copy_left:
        copy.start()

    with jax.named_scope("barrier"):
        pl.semaphore_wait(barrier, 3 - jnp.where(zed < 2, 1, 0) + jnp.where(first, others, 0))

    @pl.when(tells_ahead)
    def _():
        pl.semaphore_signal(later_sem, inc=1, device_id=(sec, ahead), device_id_type=MESH)

    @pl.when(tells_behind)
    def _():
        pl.semaphore_signal(later_sem, inc=1, device_id=(sec, behind), device_id_type=MESH)


    for offset in OFFSETS:

        @pl.when(jnp.logical_not(has_sector(-offset)))
        def _():
            inbox[pl.ds(2 * offset + 4, 2)] = jnp.zeros((2, *inbox.shape[1:]), F32)
            inmid[pl.ds(2 * offset + 4, 2)] = jnp.zeros((2, *inmid.shape[1:]), F32)
            inlast[pl.ds(2 * offset + 4, 2)] = jnp.zeros((2, *inlast.shape[1:]), F32)

    def state_hop(way, dist, part_rows, index):
        sign = 1 if way == 0 else -1
        owner = lax.rem(pan - sign * 2 * (dist - 1) + panels, panels)
        return pltpu.make_async_remote_copy(
            src_ref=mbuf.at[owner, part_rows],
            dst_ref=mbuf.at[owner, part_rows],
            send_sem=s_send.at[way],
            recv_sem=s_recv.at[way, index],
            device_id=(sec, ahead if way == 0 else behind),
            device_id_type=MESH,
        )

    def state_arrival(way, dist, part_rows, index):
        sign = 1 if way == 0 else -1
        owner = lax.rem(pan - sign * 2 * dist + 2 * panels, panels)
        return pltpu.make_async_remote_copy(
            src_ref=mbuf.at[owner, part_rows],
            dst_ref=mbuf.at[owner, part_rows],
            send_sem=s_send.at[way],
            recv_sem=s_recv.at[way, index],
            device_id=(sec, ahead if way == 0 else behind),
            device_id_type=MESH,
        )

    def state_rows(way, dist):
        if dist < 4:
            return pl.ds(0, rows)
        return pl.ds(way * half, half)

    def slot(way, dist):
        if dist == 0:
            return 0
        return ring_size - dist if way == 0 else dist

    def goes(way, piece, target):
        target = lax.rem(target + ring_size, ring_size)
        ahead_pieces = PIECES // 2
        for place, pieces in enumerate(EARLY_PIECES):
            ahead_pieces = jnp.where(target == place, pieces, ahead_pieces)
        return piece < ahead_pieces if way == 0 else piece >= ahead_pieces

    def ring_hop(way, dist, chunk):
        if dist < 4:
            piece = pl.ds(chunk * per_chunk, per_chunk)
        else:
            piece = pl.ds(last_from[chunk], LAST_TERMS[chunk])
        return pltpu.make_async_remote_copy(
            src_ref=ring.at[slot(way, dist - 1), piece],
            dst_ref=ring.at[slot(way, dist), piece],
            send_sem=r_send.at[way] if dist < 4 else l_send.at[way],
            recv_sem=r_recv.at[way, (dist - 1) * CHUNKS + chunk] if dist < 4 else l_recv.at[chunk],
            device_id=(sec, ahead if way == 0 else behind),
            device_id_type=MESH,
        )

    def send_state(dist):
        for way in range(2):
            state_hop(way, dist, state_rows(way, dist), dist - 1).start()

    def wait_state(dist):
        for way in range(2):
            state_arrival(way, dist, state_rows(way, dist), dist - 1).wait_recv()

    def hop(dist, way):
        state_arrival(way, dist, state_rows(way, dist), dist - 1).wait_recv()
        state_hop(way, dist + 1, state_rows(way, dist + 1), dist).start()
        if way == 0:
            ring_hop(way, 1, dist).start()
        else:

            @pl.when(jnp.logical_not(leads))
            def _():
                ring_hop(way, 1, dist).start()

            if dist + 1 < CHUNKS:

                @pl.when(leads)
                def _():
                    ring_hop(way, 1, dist + 1).start()

    leads = (zed == 1) | (zed == 2)

    def send_own(chunk):
        for way in range(2):
            ring_hop(way, 1, chunk).start()

    def service(dist, chunk, ways=(1, 0)):
        for way in ways:
            ring_hop(way, dist, chunk).wait_recv()
            if dist < 3:
                ring_hop(way, dist + 1, chunk).start()
            else:
                for piece in range(PIECES):
                    if (last_from[piece] + LAST_TERMS[piece] - 1) // per_chunk == chunk:

                        @pl.when(goes(way, piece, zed + 1 if way == 0 else zed - 1))
                        def _():
                            ring_hop(way, 4, piece).start()

    def first_sends(way):
        state_hop(way, 1, state_rows(way, 1), 0).start()
        ring_hop(way, 1, 0).start()
        if way == 1:

            @pl.when(leads)
            def _():
                ring_hop(1, 1, 1).start()

    with jax.named_scope("own_state"):
        copy_state.wait()
        copy_right.wait()

    @pl.when(zed == 0)
    def _():
        first_sends(0)
        pl.semaphore_wait(later_sem, 1)
        first_sends(1)

    @pl.when(zed == 1)
    def _():
        first_sends(1)
        pl.semaphore_wait(later_sem, 1)
        first_sends(0)

    @pl.when(zed > 1)
    def _():
        first_sends(1)
        first_sends(0)

    for copy in tables:
        copy.wait()
    live = sdims[0, 0]
    lanes = channels * half
    slot_row = (vout[...] - sec + 2).astype(F32)
    table = jnp.concatenate(
        [slot_row, vterm[...].astype(F32), vcoup[...].astype(F32), jnp.zeros((5, channels), F32)], axis=0
    ).astype(BF16)
    chan_of_lane = lax.broadcasted_iota(jnp.int32, (channels, lanes), 1) // half
    chan = lax.broadcasted_iota(jnp.int32, (channels, lanes), 0)
    spread = jnp.where(chan_of_lane == chan, 1.0, 0.0).astype(BF16)
    wide = jnp.dot(table, spread, preferred_element_type=F32)
    row_in_half = lax.rem(lax.broadcasted_iota(jnp.int32, (1, lanes), 1), half).astype(F32)
    target = (wide[1:2] * 5.0 + wide[0:1]) * float(half) + row_in_half
    weight = wide[2:3]

    tile = 256

    def combine(step):
        at = lax.broadcasted_iota(jnp.int32, (tile, lanes), 0).astype(F32) + float(step * tile)
        kron = jnp.where(at == target, weight, 0.0).astype(BF16)
        for g in range(2):
            made = jnp.dot(kron, lbuf[g].reshape(lanes, width), preferred_element_type=F32).astype(BF16)
            groups = tile // half
            cbuf[pl.ds(step * groups, groups), g] = made.reshape(groups, half, width)

    pltpu.make_async_copy(lbuf, lbuf, local_sem.at[2]).wait()
    with jax.named_scope("combine_a"):
        combine(0)
        combine(1)
    with jax.named_scope("hop_1"):
        hop(1, 1)
        hop(1, 0)
    combine(2)
    combine(3)
    with jax.named_scope("hop_2"):
        hop(2, 1)
        hop(2, 0)
    combine(4)
    with jax.named_scope("hop_3"):
        hop(3, 1)
        service(1, 0, (1,))
        service(1, 1, (1,))
        hop(3, 0)
    service(1, 0, (0,))
    service(1, 1, (0,))
    with jax.named_scope("hop_4"):
        wait_state(4)

    def pair_copy(step):
        return pltpu.make_async_remote_copy(
            src_ref=mbuf.at[2 * step + core],
            dst_ref=mbuf.at[2 * step + core],
            send_sem=pair_send,
            recv_sem=pair_recv,
            device_id=(sec, partner),
            device_id_type=MESH,
        )

    for step in range(ring_size):
        pair_copy(step).start()
    for offset in OFFSETS:

        @pl.when(first & has_sector(offset))
        def _():
            for other in (pan, partner):
                pl.semaphore_signal(
                    column_sem, inc=1, device_id=(sector_at(offset), other), device_id_type=MESH
                )

    pair_all = pltpu.make_async_remote_copy(
        src_ref=mbuf.at[pl.ds(0, ring_size)],
        dst_ref=mbuf.at[pl.ds(0, ring_size)],
        send_sem=pair_send,
        recv_sem=pair_recv,
        device_id=(sec, partner),
        device_id_type=MESH,
    )
    pair_all.wait_recv()

    row_at = lax.broadcasted_iota(jnp.int32, (width, width), 0)
    col_at = lax.broadcasted_iota(jnp.int32, (width, width), 1)
    masked = jnp.where(
        (row_at < live) & (col_at < live), mbuf[...].reshape(width, width), jnp.zeros((), BF16)
    )
    mfull[...] = masked
    group = 4
    for step in range(terms // group):
        block = cbuf[pl.ds(step * group * 5, group * 5)].reshape(group * 5 * rows, width)
        made = jnp.dot(block, mfull[...], preferred_element_type=F32).astype(BF16)
        xbuf[pl.ds(step * group, group), core] = made.reshape(group, 5 * rows, width)
        if step % 2:
            service(1, 2 + step // 2)
        pltpu.make_async_remote_copy(
            src_ref=xbuf.at[pl.ds(step * group, group), core],
            dst_ref=xbuf.at[pl.ds(step * group, group), core],
            send_sem=x_send,
            recv_sem=x_recv,
            device_id=(sec, partner),
            device_id_type=MESH,
        ).start()
    x_all = pltpu.make_async_remote_copy(
        src_ref=xbuf.at[:, core],
        dst_ref=xbuf.at[:, core],
        send_sem=x_send,
        recv_sem=x_recv,
        device_id=(sec, partner),
        device_id_type=MESH,
    )

    @pl.when(first)
    def _():
        pl.semaphore_wait(column_sem, others)
        for step in range(1, ring_size):
            pl.semaphore_signal(
                ready_sem, inc=1, device_id=(sec, 2 * step + core), device_id_type=MESH
            )

    part[...] = jnp.zeros(part.shape, F32)
    x_all.wait_recv()

    def contract(slots, which, held):
        blocks = []
        for w in which:
            pieces = [ring[k, w] for k in slots]
            blocks.append(pieces[0] if len(pieces) == 1 else jnp.concatenate(pieces, axis=0))
        totals = []
        for owner in range(2):
            total = None if held is None else held[owner]
            for w, block in zip(which, blocks):
                product = nt_dot(xbuf[w, owner], block)
                total = product if total is None else total + product
            totals.append(total)
        return totals

    def place(slots, totals):
        for owner, total in enumerate(totals):
            for i, k in enumerate(slots):
                piece = total[:, i * cols : (i + 1) * cols].reshape(5, rows, cols)
                part[pl.ds(owner * 5, 5), :, pl.ds(k * cols, cols)] = piece

    def keep_in(acc, totals):
        for owner, total in enumerate(totals):
            acc[owner] = total

    def pack(total):
        total = total.reshape(5, rows // 8, 8, cols)
        return jnp.concatenate([total[:, i] for i in range(rows // 8)], axis=2)

    def unpack(packed):
        return jnp.concatenate([packed[:, i * cols : (i + 1) * cols] for i in range(rows // 8)], axis=0)

    def exchange(source, landing, send_sem, recv_sem):
        def copy_to(which, j):
            return pltpu.make_async_remote_copy(
                src_ref=source.at[which * 5 + j],
                dst_ref=landing.at[2 * j + core],
                send_sem=send_sem,
                recv_sem=recv_sem,
                device_id=(sector_at(j - 2), 2 * zed + which),
                device_id_type=MESH,
            )

        def start():
            for j in (0, 4, 1, 3):

                @pl.when(has_sector(j - 2))
                def _():
                    for which in range(2):
                        copy_to(which, j).start()

            copy_to(1 - core, 2).start()

        def wait_all(wait):
            for count in (4, 6, 8):

                @pl.when(others == count)
                def _():
                    wait(
                        pltpu.make_async_remote_copy(
                            src_ref=source.at[pl.ds(0, count + 1)],
                            dst_ref=landing.at[pl.ds(0, count + 1)],
                            send_sem=send_sem,
                            recv_sem=recv_sem,
                            device_id=(sec, partner),
                            device_id_type=MESH,
                        )
                    )

        def wait_recv():
            wait_all(lambda copy: copy.wait_recv())

        def wait_send():
            wait_all(lambda copy: copy.wait_send())

        return start, wait_recv, wait_send

    def sum_of(landing, cls):
        total = landing[cls]
        for j in range(1, 5):
            total = total + landing[2 * j + cls]
        return total

    start_a, recv_a, sent_a = exchange(part, inbox, a_send, a_recv)
    start_m, recv_m, sent_m = exchange(mid, inmid, m_send, m_recv)
    start_b, recv_b, sent_b = exchange(last, inlast, b_send, b_recv)

    def chunk_terms(chunk):
        return range(chunk * per_chunk, (chunk + 1) * per_chunk)

    with jax.named_scope("contract_a"):
        place((0, 1, 7), contract((0, 1, 7), range(terms), None))
    with jax.named_scope("ring_2"):
        for chunk in range(CHUNKS):
            service(2, chunk)
            totals = contract((2, 6), chunk_terms(chunk), acc2 if chunk else None)
            if chunk < CHUNKS - 1:
                keep_in(acc2, totals)
            else:
                place((2, 6), totals)
    with jax.named_scope("ring_3"):
        for chunk in range(CHUNKS):
            service(3, chunk)
            if chunk == 0:

                @pl.when(jnp.logical_not(first))
                def _():
                    pl.semaphore_wait(ready_sem, 1)

                start_a()
            keep_in(acc3, contract((3, 5), chunk_terms(chunk), acc3 if chunk else None))
        for owner in range(2):
            for i in range(2):
                mid[pl.ds(owner * 5, 5), pl.ds(8 * i, 8)] = pack(acc3[owner, :, pl.ds(i * cols, cols)])

    def by_final_step(step):
        return [
            w
            for piece in (step, PIECES // 2 + step)
            for w in range(last_from[piece], last_from[piece] + LAST_TERMS[piece])
        ]

    def final_wait(step):
        for piece in (step, PIECES // 2 + step):
            ring_hop(0, 4, piece).wait_recv()

    final_wait(0)
    start_m()
    keep_in(acc4, contract((4,), by_final_step(0), None))
    for step in range(1, PIECES // 2 - 1):
        final_wait(step)
        keep_in(acc4, contract((4,), by_final_step(step), acc4))
    with jax.named_scope("final_wait"):
        final_wait(PIECES // 2 - 1)
    with jax.named_scope("last"):
        totals = contract((4,), by_final_step(PIECES // 2 - 1), acc4)
        for owner in range(2):
            last[pl.ds(owner * 5, 5)] = pack(totals[owner])
        start_b()

    recv_a()
    inbox[4 + core] = part[core * 5 + 2]
    inmid[4 + core] = mid[core * 5 + 2]
    inlast[4 + core] = last[core * 5 + 2]
    recv_m()
    sums = []
    for cls in range(2):
        total = sum_of(inbox, cls)
        extra = sum_of(inmid, cls)
        total = jnp.concatenate(
            [
                total[:, : 3 * cols],
                unpack(extra[:8]),
                total[:, 4 * cols : 5 * cols],
                unpack(extra[8:]),
                total[:, 6 * cols :],
            ],
            axis=1,
        )
        sums.append(pltpu.roll(total, zed * cols, axis=1))
    pieces = []
    for k in range(ring_size):
        for cls in range(2):
            pieces.append(sums[cls][:, k * cols : (k + 1) * cols])
    early = jnp.concatenate(pieces, axis=1)
    lane = lax.broadcasted_iota(jnp.int32, (rows, width), 1)
    here = lane // (2 * cols) == lax.rem(zed + 4, ring_size)
    with jax.named_scope("sent"):
        for way in range(2):
            pltpu.make_async_remote_copy(
                src_ref=mbuf.at[pl.ds(0, 7), pl.ds(0, half)],
                dst_ref=mbuf.at[pl.ds(0, 7), pl.ds(0, half)],
                send_sem=s_send.at[way],
                recv_sem=s_recv.at[way, 0],
                device_id=(sec, partner),
                device_id_type=MESH,
            ).wait_send()
            pltpu.make_async_remote_copy(
                src_ref=ring.at[pl.ds(0, 3)],
                dst_ref=ring.at[pl.ds(0, 3)],
                send_sem=r_send.at[way],
                recv_sem=r_recv.at[way, 0],
                device_id=(sec, partner),
                device_id_type=MESH,
            ).wait_send()
            reached = lax.rem(zed + (1 if way == 0 else ring_size - 1), ring_size)
            for place, ahead_pieces in enumerate((*EARLY_PIECES, PIECES // 2)):
                is_target = reached == place if place < len(EARLY_PIECES) else reached >= place
                count = sum(LAST_TERMS[:ahead_pieces] if way == 0 else LAST_TERMS[ahead_pieces:])

                @pl.when(is_target)
                def _():
                    pltpu.make_async_remote_copy(
                        src_ref=ring.at[0, pl.ds(0, count)],
                        dst_ref=ring.at[0, pl.ds(0, count)],
                        send_sem=l_send.at[way],
                        recv_sem=l_recv.at[0],
                        device_id=(sec, partner),
                        device_id_type=MESH,
                    ).wait_send()

        pair_all.wait_send()
        x_all.wait_send()
        sent_a()
        sent_m()
        sent_b()
    with jax.named_scope("recv_b"):
        recv_b()
    with jax.named_scope("finish"):
        lasts = [unpack(sum_of(inlast, cls)) for cls in range(2)]
        late = jnp.concatenate(lasts * (width // (2 * cols)), axis=1)
        out_ref[0] = early + jnp.where(here, late, 0.0)


def on_device(
    wave_state, right_blocks, left_blocks, coupling, channel_term, channel_out, sector_dims
):
    _, rows, width = wave_state.shape
    _, terms, _, cols = right_blocks.shape
    channels = left_blocks.shape[0]
    panels = lax.axis_size("pan")
    ring_size = panels // 2
    half = rows // 2
    right = jnp.swapaxes(right_blocks[0], 1, 2)
    dma = pltpu.SemaphoreType.DMA
    applied = pl.pallas_call(
        kernel,
        out_shape=pltpu.VMEM((1, rows, width), F32),
        in_specs=[pl.BlockSpec(memory_space=pltpu.HBM)] * 7,
        out_specs=pl.BlockSpec(memory_space=pltpu.VMEM),
        scratch_shapes=[
            pltpu.VMEM((ring_size, terms, cols, width), BF16),
            pltpu.VMEM((panels, rows, width), BF16),
            pltpu.VMEM((width, width), BF16),
            pltpu.VMEM((2, channels, half, width), BF16),
            pltpu.VMEM((5 * terms, 2, half, width), BF16),
            pltpu.VMEM((terms, 2, 5 * rows, width), BF16),
            pltpu.VMEM((10, rows, ring_size * cols), F32),
            pltpu.VMEM((2, 5 * rows, 2 * cols), F32),
            pltpu.VMEM((2, 5 * rows, 2 * cols), F32),
            pltpu.VMEM((2, 5 * rows, cols), F32),
            pltpu.VMEM((10, rows, ring_size * cols), F32),
            pltpu.VMEM((10, 16, rows // 8 * cols), F32),
            pltpu.VMEM((10, 16, rows // 8 * cols), F32),
            pltpu.VMEM((10, 8, rows // 8 * cols), F32),
            pltpu.VMEM((10, 8, rows // 8 * cols), F32),
            pltpu.VMEM((1, channels), BF16),
            pltpu.VMEM((1, channels), jnp.int32),
            pltpu.VMEM((1, channels), jnp.int32),
            pltpu.SMEM((1, 1), jnp.int32),
            dma((7,)),
            dma((2,)),
            dma((2, 4)),
            dma((2,)),
            dma((2, 3 * CHUNKS)),
            dma((2,)),
            dma((PIECES,)),
            dma(()),
            dma(()),
            dma(()),
            dma(()),
            dma(()),
            dma(()),
            dma(()),
            dma(()),
            dma(()),
            dma(()),
            pltpu.SemaphoreType.REGULAR,
            pltpu.SemaphoreType.REGULAR,
            pltpu.SemaphoreType.REGULAR,
        ],
        compiler_params=pltpu.CompilerParams(
            collective_id=0, has_side_effects=True, vmem_limit_bytes=60 * 1024 * 1024
        ),
        name="sector_step",
    )(
        wave_state,
        right,
        left_blocks,
        coupling[None],
        channel_term[None],
        channel_out[None],
        sector_dims[None],
    )
    live = sector_dims[0]
    row_ids = lax.axis_index("pan") * rows + lax.iota(jnp.int32, rows)
    kept_mask = (row_ids[:, None] < live) & (lax.iota(jnp.int32, width)[None, :] < live)
    return jnp.where(kept_mask[None], applied, jnp.zeros((), F32))


def solution(mesh):
    return jax.shard_map(
        on_device,
        mesh=mesh,
        in_specs=(
            P("sec", "pan", None),
            P("sec", None, None, "pan"),
            P("sec", "pan", None),
            P("sec"),
            P("sec"),
            P("sec"),
            P("sec"),
        ),
        out_specs=P("sec", "pan", None),
        check_vma=False,
    )
```
